512 devices in a mesh: vox: 64 (over z, x, core), subj: 8 (over y).
Axes of the slice: x: 4, y: 8, z: 8, core: 2. Of those that a mesh axis runs over, the one named last changes fastest.
Arguments:
- series: bfloat16 [32, 16384, 512], P('subj', 'vox'), may hold values from -6 to 6
- live_mask: int32 [16384], P('vox'), may hold values from 0 to 1, as said below
- neighbours: int32 [16384, 13], P('vox'), may hold values from -1 to 510, as said below
- start_vectors: float32 [16384, 64], P('vox'), may hold values from -60 to 60
Outputs:
- embedding: float32 [16384, 64], P('vox')
The draws below stay inside these ranges and needn't reach their ends.
Inputs may be any that keep to these rules, and one draw needn't show every extreme that they name: `live_mask`: within each aligned block of 128 voxel slots the live slots are a leading run of 1 to 128 slots. `neighbours`: slot n of voxel i names voxel (i // 256 - 1) * 256 + n, which is live and lies before i; the entries of a row are distinct or -1; rows of dead voxels are all -1; rows of the first 256 voxels name no slot under 256.
All inputs are finite; a program needn't handle non-finite values.
Results may differ from the reference program's by a relative error of at most 0.0024.
Values may be sent and summed in bfloat16 or wider, within the bound.
A program may use at most 64 MiB of HBM per device.

```python
import math
import jax
import jax.numpy as jnp
from jax import lax

VOX_DEV = 256
FRAMES = 512
VECS = 64
OFFSETS = 13
BLOCK = 128
ITERS = 3
VOXELS = 16384
SUBJECTS = 32


def brain_layout(key):
    first, second = jax.random.split(jax.random.fold_in(key, 7))
    blocks = VOXELS // BLOCK
    filled = jax.random.randint(first, (blocks,), 1, BLOCK + 1)
    within = jnp.arange(BLOCK, dtype=jnp.int32)
    living = (within[None, :] < filled[:, None]).reshape(-1).astype(jnp.int32)
    position = jnp.arange(VOXELS, dtype=jnp.int32)
    stride = VOX_DEV // OFFSETS
    lowest = jnp.arange(OFFSETS, dtype=jnp.int32) * stride + 1
    distance = lowest[None, :] + jax.random.randint(second, (VOXELS, OFFSETS), 0, stride)
    target = position[:, None] - distance
    usable = (target >= 0) & (living[jnp.maximum(target, 0)] == 1) & (living[:, None] == 1)
    local_slot = VOX_DEV + (position % VOX_DEV)[:, None] - distance
    return (living, jnp.where(usable, local_slot, -1).astype(jnp.int32))


def draw_live_mask(key, part):
    return brain_layout(key)[0]


def draw_neighbours(key, part):
    return brain_layout(key)[1]


def draw_start_vectors(key, part):
    first = jax.random.fold_in(jax.random.fold_in(key, 11), 0)
    fraction = jnp.arange(VOXELS, dtype=jnp.float32) / VOXELS
    noise = jnp.clip(jax.random.normal(first, (VOXELS, VECS), jnp.float32), -6.0, 6.0)
    rows = (1.0 + 3.0 * fraction)[:, None]
    return noise * rows


def block_levels(stream_key, shape, pieces, low, largest):
    def one(dim, blocks):
        draws = jax.random.uniform(jax.random.fold_in(jax.random.fold_in(stream_key, 6), dim), (blocks,), jnp.float32, low / len(pieces), largest / len(pieces))
        return jnp.repeat(jnp.exp(draws), shape[dim] // blocks).reshape((-1,) + (1,) * (len(shape) - dim - 1))

    level = one(*pieces[0])
    for cut in pieces[1:]:
        level = level * one(*cut)
    return level


def scatter_about(stream_key, shape, scale, bound, cuts=(), kind=jnp.bfloat16):
    result = scale * jax.random.normal(stream_key, shape, jnp.float32)
    if cuts:
        result = result * block_levels(stream_key, shape, cuts, -0.22, 0.18)
    return jnp.clip(result, -bound, bound).astype(kind)


def setup_inputs(seed: int = 0) -> dict:
    splits = jax.random.split(jax.random.key(seed), 5)
    return {
        "series": scatter_about(splits[0], (SUBJECTS, VOXELS, FRAMES), 1.0, 6.0, ((0, 8), (1, 64))),
        "live_mask": draw_live_mask(jax.random.fold_in(splits[4], 71), 0),
        "neighbours": draw_neighbours(jax.random.fold_in(splits[4], 71), 0),
        "start_vectors": draw_start_vectors(jax.random.fold_in(splits[4], 71), 0),
    }


def standard(block):
    values = block.astype(jnp.float32)
    center = values - lax.optimization_barrier(jnp.mean(values, axis=-1, keepdims=True))
    spread = lax.optimization_barrier(jnp.mean(center * center, axis=-1, keepdims=True))
    return (center * lax.rsqrt(spread + 1e-05)).astype(jnp.bfloat16)

def reference(series, live_mask, neighbours, start_vectors):
    position = jnp.arange(VOXELS, dtype=jnp.int32)
    present = neighbours >= 0
    global_index = jnp.where(present, ((position // VOX_DEV - 1) * VOX_DEV)[:, None] + neighbours, 0).astype(jnp.int32)

    def one_subject(summed, block):
        zscored = standard(block).astype(jnp.float32)
        columns = []
        for offset in range(OFFSETS):
            columns.append(lax.optimization_barrier(jnp.sum(zscored * zscored[global_index[:, offset]], axis=1)))
        return (summed + jnp.stack(columns, axis=1), None)
    summed, _ = lax.scan(one_subject, jnp.zeros((VOXELS, OFFSETS), jnp.float32), series)
    weight = jnp.where(present, jnp.exp(0.5 * summed / math.sqrt(FRAMES * SUBJECTS)), 0.0)
    flat_index = global_index.reshape(-1)
    degree = 1.0 + lax.optimization_barrier(jnp.sum(weight, axis=1)) + jax.ops.segment_sum(weight.reshape(-1), flat_index, num_segments=VOXELS)
    living = live_mask.astype(jnp.float32)
    scaling = living * lax.rsqrt(degree)
    vectors = living[:, None] * start_vectors
    for repeat in range(ITERS):
        scaled = scaling[:, None] * vectors
        forward = lax.optimization_barrier(jnp.sum(weight[:, :, None] * scaled[global_index], axis=1))
        returns = jax.ops.segment_sum((weight[:, :, None] * scaled[:, None, :]).reshape(-1, VECS), flat_index, num_segments=VOXELS)
        images = 0.5 * (vectors + scaling[:, None] * (scaled + forward + returns))
        gram_matrix = jnp.dot(images.T, images, precision=lax.Precision.HIGHEST)
        factor = jnp.linalg.cholesky(gram_matrix)
        vectors = lax.linalg.triangular_solve(factor, images, left_side=False, lower=True, transpose_a=True)
    return vectors
```

```python
import functools
import math

import jax
import jax.numpy as jnp
from jax import lax
from jax.experimental import pallas as pl
from jax.experimental.pallas import tpu as pltpu
from jax.sharding import PartitionSpec as P

ITERS = 3
HIGHEST = lax.Precision.HIGHEST
NN = (((1,), (0,)), ((), ()))
NT = (((1,), (1,)), ((), ()))


def matmul(left, right, dims, precision=None):
    return lax.dot_general(
        left, right, dims, precision=precision, preferred_element_type=jnp.float32
    )


def split(values):
    high = values.astype(jnp.bfloat16)
    low = (values - high.astype(jnp.float32)).astype(jnp.bfloat16)
    return high, low


def factor_inverse(rows):
    total, width = rows.shape
    sublane = lax.broadcasted_iota(jnp.int32, (8, width), 0)
    done = []
    for first in range(0, total, 8):
        left = total - first
        cols = [
            jnp.broadcast_to(rows[:, first + c : first + c + 1], (left, width))
            for c in range(8)
        ]
        block = jnp.zeros((8, width), jnp.float32)
        for c in range(8):
            root = lax.rsqrt(cols[c][c : c + 1, :])
            lower = cols[c] * root
            pivot = rows[c : c + 1, :] * root
            block = jnp.where(sublane == c, pivot, block)
            rows = rows - lower * pivot
            for other in range(c + 1, 8):
                cols[other] = cols[other] - lower * lower[other : other + 1, :]
        done.append(block)
        rows = rows[8:]
    return jnp.concatenate(done, axis=0)


def kernel(
    sizes,
    series_ref,
    mask_ref,
    near_ref,
    start_ref,
    out_ref,
    raw,
    zown,
    zprev,
    near,
    live,
    begin,
    corr,
    part,
    parts,
    ghigh,
    glow,
    owed,
    owing,
    scale_row,
    image,
    ahead,
    ahead_in,
    back,
    back_in,
    gram,
    stage1,
    half,
    stage2,
    whole,
    other,
    in_sems,
    z_send,
    z_recv,
    part_send,
    part_recv,
    owed_sems,
    halo_send,
    halo_recv,
    s1_send,
    s1_recv,
    s2_send,
    s2_recv,
    s3_sems,
):
    groups, plane, planes, scale_factor = sizes
    count = plane * planes
    subjects, voxels, frames = series_ref.shape
    offsets = near_ref.shape[0]
    vecs = start_ref.shape[0]
    me = lax.axis_index("vox")
    group = lax.axis_index("subj")
    spot = lax.rem(me, plane)
    level = me // plane
    core = lax.rem(me, 2)
    following = lax.rem(me + 1, count)
    previous = lax.rem(me + count - 1, count)
    partner = me + 1 - 2 * core

    plane_peers = [lax.rem(spot + d, plane) for d in range(1, plane)]
    level_peers = [lax.rem(level + d, planes) for d in range(1, planes)]
    group_peers = [lax.rem(group + d, groups) for d in range(1, groups)]

    loads = [
        pltpu.make_async_copy(series_ref.at[s], raw.at[s], in_sems.at[s])
        for s in range(subjects)
    ]
    small = [
        pltpu.make_async_copy(near_ref, near, in_sems.at[subjects]),
        pltpu.make_async_copy(mask_ref, live, in_sems.at[subjects + 1]),
        pltpu.make_async_copy(start_ref, begin, in_sems.at[subjects + 2]),
    ]
    for load in loads + small:
        load.start()

    barrier = pltpu.get_barrier_semaphore()
    targets = [{"vox": following}, {"vox": previous}]
    targets += [{"vox": level * plane + p} for p in plane_peers]
    targets += [{"vox": p * plane + spot} for p in level_peers]
    targets += [{"subj": p} for p in group_peers]
    for target in targets:
        pl.semaphore_signal(
            barrier, inc=1, device_id=target, device_id_type=pl.DeviceIdType.MESH
        )

    def remote(src, dst, send, recv, target):
        return pltpu.make_async_remote_copy(
            src_ref=src,
            dst_ref=dst,
            send_sem=send,
            recv_sem=recv,
            device_id=target,
            device_id_type=pl.DeviceIdType.MESH,
        )

    step = 32
    z_copies = []
    for s in range(subjects):
        loads[s].wait()

        @pl.loop(0, voxels // step)
        def _(r):
            rows = pl.ds(pl.multiple_of(r * step, step), step)
            values = raw[s, rows, :].astype(jnp.float32)
            center = values - jnp.mean(values, axis=-1, keepdims=True)
            spread = jnp.mean(center * center, axis=-1, keepdims=True)
            zown[s, rows, :] = (center * lax.rsqrt(spread + 1e-05)).astype(jnp.bfloat16)

        if s == 0:
            pl.semaphore_wait(barrier, len(targets))
        copy = remote(
            zown.at[s], zprev.at[s], z_send.at[s], z_recv.at[s], {"vox": following}
        )
        copy.start()
        z_copies.append(copy)
        local = matmul(zown[s], zown[s], NT)
        if s == 0:
            corr[voxels:, :] = local
        else:
            corr[voxels:, :] += local
    for load in small:
        load.wait()

    tile = lax.broadcasted_iota(jnp.int32, (8, voxels), 0)
    slots = [jnp.broadcast_to(near[k : k + 1, :], (8, voxels)) for k in range(offsets)]

    def picked(first, last, sums):
        def body(r, sums):
            ids = tile + r * 8
            values = corr[pl.ds(pl.multiple_of(r * 8, 8), 8), :]
            return tuple(
                total + jnp.where(ids == slots[k], values, 0.0)
                for k, total in enumerate(sums)
            )

        return lax.fori_loop(first // 8, last // 8, body, sums, unroll=2)

    sums = tuple(jnp.zeros((8, voxels), jnp.float32) for _ in range(offsets))
    sums = picked(voxels, 2 * voxels, sums)
    for s in range(subjects):
        z_copies[s].wait_recv()
        cross = matmul(zprev[s], zown[s], NT)
        if s == 0:
            corr[:voxels, :] = cross
        else:
            corr[:voxels, :] += cross
    sums = picked(0, voxels, sums)
    part[...] = jnp.zeros(part.shape, jnp.float32)
    for k in range(offsets):
        part[k : k + 1, :] = jnp.sum(sums[k], axis=0, keepdims=True)

    part_copies = []
    for d, peer in enumerate(group_peers):
        copy = remote(
            part, parts.at[group], part_send.at[d], part_recv.at[group], {"subj": peer}
        )
        copy.start()
        part_copies.append(copy)
    parts[group] = part[...]
    vectors = live[...].astype(jnp.float32) * begin[...]
    for d, peer in enumerate(group_peers):
        remote(
            part, parts.at[peer], part_send.at[d], part_recv.at[peer], {"subj": peer}
        ).wait_recv()
    summed = parts[0]
    for g in range(1, groups):
        summed = summed + parts[g]
    weight = [
        jnp.where(
            near[k : k + 1, :] >= 0, jnp.exp(scale_factor * summed[k : k + 1, :]), 0.0
        )
        for k in range(offsets)
    ]
    listed = weight[0]
    for k in range(1, offsets):
        listed = listed + weight[k]
    spread_weight = [jnp.broadcast_to(w, (8, voxels)) for w in weight]

    @pl.loop(0, 2 * voxels // 16)
    def _(r):
        tiles = []
        for h in range(2):
            ids = tile + (r * 16 + h * 8)
            entry = jnp.zeros((8, voxels), jnp.float32)
            for k in range(offsets):
                entry = jnp.where(ids == slots[k], spread_weight[k], entry)
            tiles.append(entry)
        high, low = split(jnp.concatenate(tiles, axis=0))
        rows = pl.ds(pl.multiple_of(r * 16, 16), 16)
        ghigh[rows, :] = high
        glow[rows, :] = low

    ones = jnp.ones((8, voxels), jnp.bfloat16)
    columns = matmul(ones, ghigh[...], NT) + matmul(ones, glow[...], NT)
    owed[...] = columns[:, :voxels]
    owed_copy = remote(owed, owing, owed_sems.at[0], owed_sems.at[1], {"vox": previous})
    owed_copy.start()
    owed_copy.wait_recv()
    degree = 1.0 + listed + columns[:1, voxels:] + owing[:1, :]
    scale_row[...] = live[...].astype(jnp.float32) * lax.rsqrt(degree)

    def halo(t):
        return (
            remote(
                ahead.at[t], ahead_in.at[t], halo_send.at[t, 0], halo_recv.at[t, 0],
                {"vox": following},
            ),
            remote(
                back.at[t], back_in.at[t], halo_send.at[t, 1], halo_recv.at[t, 1],
                {"vox": previous},
            ),
        )

    def send_halo(t, current):
        scaled = scale_row[...] * current
        ahead[t] = scaled
        forward, backward = halo(t)
        forward.start()
        high, low = split(scaled)
        both = jnp.concatenate([high, low], axis=0)
        first = matmul(both, ghigh[:voxels, :], NT)
        back[t] = first[:vecs] + first[vecs:] + matmul(high, glow[:voxels, :], NT)
        backward.start()

    def apply(t, current):
        scaled = scale_row[...] * current
        high, low = split(scaled)
        both = jnp.concatenate([high, low], axis=0)
        mine = matmul(both, ghigh[voxels:, :], NT) + matmul(both, ghigh[voxels:, :], NN)
        rest = matmul(high, glow[voxels:, :], NT) + matmul(high, glow[voxels:, :], NN)
        for copy in halo(t):
            copy.wait_recv()
        early_high, early_low = split(ahead_in[t])
        early = jnp.concatenate([early_high, early_low], axis=0)
        mine = mine + matmul(early, ghigh[:voxels, :], NN)
        rest = rest + matmul(early_high, glow[:voxels, :], NN)
        total = scaled + mine[:vecs] + mine[vecs:] + rest + back_in[t]
        return 0.5 * (current + scale_row[...] * total)

    send_halo(0, vectors)
    image[...] = apply(0, vectors)

    lane = lax.broadcasted_iota(jnp.int32, (vecs // 2, 2 * vecs), 1)
    row = lax.broadcasted_iota(jnp.int32, (vecs // 2, 2 * vecs), 0)
    quarter = vecs // 4

    def stage1_copy(t, d, arriving=False):
        peer = plane_peers[d]
        source = gram.at[t, pl.ds(pl.multiple_of(lax.rem(peer, 2) * quarter, quarter), quarter)]
        target = {"vox": level * plane + peer}
        slot = peer if arriving else spot
        return remote(source, stage1.at[t, slot], s1_send.at[t, d], s1_recv.at[t, slot], target)

    def stage2_copy(t, d, arriving=False):
        peer = level_peers[d]
        target = {"vox": peer * plane + spot}
        slot = peer if arriving else level
        return remote(half.at[t], stage2.at[t, slot], s2_send.at[t, d], s2_recv.at[t, slot], target)

    def stage3_copy(t):
        return remote(whole.at[t], other.at[t], s3_sems.at[t, 0], s3_sems.at[t, 1], {"vox": partner})

    def iterate(t):
        current = image[...]
        twice = jnp.concatenate([current, current], axis=0)
        product = matmul(current, twice, NT, HIGHEST)
        packed = jnp.where(lane < vecs, product[: vecs // 2], product[vecs // 2 :])
        gram[t] = packed
        for d in range(plane - 1):
            stage1_copy(t, d).start()
        own = pl.ds(pl.multiple_of(core * quarter, quarter), quarter)
        stage1[t, spot] = gram[t, own]

        @pl.when(t < ITERS - 1)
        def _():
            send_halo(t + 1, current)

        for d in range(plane - 1):
            stage1_copy(t, d, True).wait_recv()
        total = stage1[t, 0]
        for p in range(1, plane):
            total = total + stage1[t, p]
        half[t] = total
        for d in range(planes - 1):
            stage2_copy(t, d).start()
        stage2[t, level] = total

        @pl.when(t < ITERS - 1)
        def _():
            image[...] = apply(t + 1, current)

        for d in range(planes - 1):
            stage2_copy(t, d, True).wait_recv()
        total = stage2[t, 0]
        for p in range(1, planes):
            total = total + stage2[t, p]
        whole[t] = total
        exchange = stage3_copy(t)
        exchange.start()
        exchange.wait_recv()
        got = other[t]
        upper = jnp.where(core == 0, total, got)
        lower = jnp.where(core == 0, got, total)
        full = jnp.concatenate([upper, lower], axis=0)
        top = jnp.where(lane < vecs, full, (lane - vecs == row).astype(jnp.float32))
        bottom = jnp.where(
            lane < vecs,
            pltpu.roll(full, vecs, 1),
            (lane - vecs == row + vecs // 2).astype(jnp.float32),
        )
        solved = factor_inverse(jnp.concatenate([top, bottom], axis=0))
        inverse = pltpu.roll(solved, vecs, 1)[:, :vecs]
        image[...] = matmul(inverse, image[...], NN, HIGHEST)

    pl.loop(0, ITERS)(iterate)
    out_ref[...] = image[...]

    for copy in z_copies + part_copies + [owed_copy]:
        copy.wait_send()
    for t in range(ITERS):
        for copy in halo(t):
            copy.wait_send()
        for d in range(plane - 1):
            stage1_copy(t, d).wait_send()
        for d in range(planes - 1):
            stage2_copy(t, d).wait_send()
        stage3_copy(t).wait_send()


def solution(mesh):
    count, groups = mesh.shape["vox"], mesh.shape["subj"]
    plane = 8 if count >= 16 else count // 2
    planes = count // plane

    def on_device(series, live_mask, neighbours, start_vectors):
        subjects, voxels, frames = series.shape
        vecs = start_vectors.shape[1]
        offsets = neighbours.shape[1]
        scale_factor = 0.5 / math.sqrt(frames * subjects * groups)
        f32, bf16, i32 = jnp.float32, jnp.bfloat16, jnp.int32
        block = (vecs, voxels)
        quarter = (vecs // 4, 2 * vecs)
        dma = pltpu.SemaphoreType.DMA
        anywhere = pl.BlockSpec(memory_space=pl.ANY)
        result = pl.pallas_call(
            functools.partial(kernel, (groups, plane, planes, scale_factor)),
            out_shape=jax.ShapeDtypeStruct(block, f32),
            in_specs=[anywhere] * 4,
            out_specs=pl.BlockSpec(memory_space=pltpu.VMEM),
            scratch_shapes=[
                pltpu.VMEM((subjects, voxels, frames), bf16),
                pltpu.VMEM((subjects, voxels, frames), bf16),
                pltpu.VMEM((subjects, voxels, frames), bf16),
                pltpu.VMEM((offsets, voxels), i32),
                pltpu.VMEM((1, voxels), i32),
                pltpu.VMEM(block, f32),
                pltpu.VMEM((2 * voxels, voxels), f32),
                pltpu.VMEM((16, voxels), f32),
                pltpu.VMEM((groups, 16, voxels), f32),
                pltpu.VMEM((2 * voxels, voxels), bf16),
                pltpu.VMEM((2 * voxels, voxels), bf16),
                pltpu.VMEM((8, voxels), f32),
                pltpu.VMEM((8, voxels), f32),
                pltpu.VMEM((1, voxels), f32),
                pltpu.VMEM(block, f32),
                pltpu.VMEM((ITERS, *block), f32),
                pltpu.VMEM((ITERS, *block), f32),
                pltpu.VMEM((ITERS, *block), f32),
                pltpu.VMEM((ITERS, *block), f32),
                pltpu.VMEM((ITERS, vecs // 2, 2 * vecs), f32),
                pltpu.VMEM((ITERS, plane, *quarter), f32),
                pltpu.VMEM((ITERS, *quarter), f32),
                pltpu.VMEM((ITERS, planes, *quarter), f32),
                pltpu.VMEM((ITERS, *quarter), f32),
                pltpu.VMEM((ITERS, *quarter), f32),
                dma((subjects + 3,)),
                dma((subjects,)),
                dma((subjects,)),
                dma((max(groups - 1, 1),)),
                dma((groups,)),
                dma((2,)),
                dma((ITERS, 2)),
                dma((ITERS, 2)),
                dma((ITERS, plane - 1)),
                dma((ITERS, plane)),
                dma((ITERS, planes - 1)),
                dma((ITERS, planes)),
                dma((ITERS, 2)),
            ],
            compiler_params=pltpu.CompilerParams(
                collective_id=0, has_side_effects=True, vmem_limit_bytes=32 << 20
            ),
        )(series, live_mask.reshape(1, voxels), neighbours.T, start_vectors.T)
        return result.T

    placed = (P("subj", "vox", None), P("vox"), P("vox", None), P("vox", None))
    return jax.shard_map(
        on_device, mesh=mesh, in_specs=placed, out_specs=P("vox", None), check_vma=False
    )
```

```python
import functools
import math

import jax
import jax.numpy as jnp
from jax import lax
from jax.experimental import pallas as pl
from jax.experimental.pallas import tpu as pltpu
from jax.sharding import PartitionSpec as P

ITERS = 3
HIGHEST = lax.Precision.HIGHEST
NN = (((1,), (0,)), ((), ()))
NT = (((1,), (1,)), ((), ()))


def matmul(left, right, dims, precision=None):
    return lax.dot_general(
        left, right, dims, precision=precision, preferred_element_type=jnp.float32
    )


def split(values):
    high = values.astype(jnp.bfloat16)
    low = (values - high.astype(jnp.float32)).astype(jnp.bfloat16)
    return high, low


def factor_inverse(rows):
    total, width = rows.shape
    sublane = lax.broadcasted_iota(jnp.int32, (8, width), 0)
    done = []
    for first in range(0, total, 8):
        left = total - first
        cols = [
            jnp.broadcast_to(rows[:, first + c : first + c + 1], (left, width))
            for c in range(8)
        ]
        block = jnp.zeros((8, width), jnp.float32)
        for c in range(8):
            root = lax.rsqrt(cols[c][c : c + 1, :])
            lower = cols[c] * root
            pivot = rows[c : c + 1, :] * root
            block = jnp.where(sublane == c, pivot, block)
            rows = rows - lower * pivot
            for other in range(c + 1, 8):
                cols[other] = cols[other] - lower * lower[other : other + 1, :]
        done.append(block)
        rows = rows[8:]
    return jnp.concatenate(done, axis=0)


def kernel(
    sizes,
    series_ref,
    mask_ref,
    near_ref,
    start_ref,
    out_ref,
    raw,
    zown,
    zahead,
    zback,
    near,
    near_next,
    live,
    begin,
    corr,
    corr_next,
    part_next,
    part_in,
    part,
    parts,
    listed,
    listed_next,
    ghigh,
    glow,
    nhigh,
    nlow,
    scale_row,
    scale_prev,
    scale_next,
    halo_out,
    from_prev,
    from_next,
    gram,
    stage1,
    half,
    stage2,
    whole,
    other,
    in_sems,
    send,
    recv,
    part_send,
    part_recv,
    halo_send,
    halo_recv,
    s1_send,
    s1_recv,
    s2_send,
    s2_recv,
    s3_sems,
):
    groups, plane, planes, scale_factor = sizes
    count = plane * planes
    subjects, voxels, frames = series_ref.shape
    offsets = near_ref.shape[0]
    vecs = start_ref.shape[0]
    halves, width = 2 * subjects, frames // 2
    passed = zahead.shape[0]
    me = lax.axis_index("vox")
    group = lax.axis_index("subj")
    spot = lax.rem(me, plane)
    level = me // plane
    core = lax.rem(me, 2)
    following = {"vox": lax.rem(me + 1, count)}
    previous = {"vox": lax.rem(me + count - 1, count)}
    partner = {"vox": me + 1 - 2 * core}

    plane_peers = [lax.rem(spot + d, plane) for d in range(1, plane)]
    level_peers = [lax.rem(level + d, planes) for d in range(1, planes)]
    group_peers = [lax.rem(group + d, groups) for d in range(1, groups)]

    order = [0] + list(range(subjects - 1, 0, -1))
    loads = [
        pltpu.make_async_copy(series_ref.at[s], raw.at[s], in_sems.at[s])
        for s in range(subjects)
    ]
    small = [
        pltpu.make_async_copy(near_ref, near, in_sems.at[subjects]),
        pltpu.make_async_copy(mask_ref, live, in_sems.at[subjects + 1]),
        pltpu.make_async_copy(start_ref, begin, in_sems.at[subjects + 2]),
    ]
    loads[0].start()
    for load in small:
        load.start()
    for s in order[1:]:
        loads[s].start()

    barrier = pltpu.get_barrier_semaphore()
    targets = [following, previous]
    targets += [{"vox": level * plane + p} for p in plane_peers]
    targets += [{"vox": p * plane + spot} for p in level_peers]
    targets += [{"subj": p} for p in group_peers]
    for target in targets:
        pl.semaphore_signal(
            barrier, inc=1, device_id=target, device_id_type=pl.DeviceIdType.MESH
        )

    def remote(src, dst, send_sem, recv_sem, target):
        return pltpu.make_async_remote_copy(
            src_ref=src,
            dst_ref=dst,
            send_sem=send_sem,
            recv_sem=recv_sem,
            device_id=target,
            device_id_type=pl.DeviceIdType.MESH,
        )

    def single(index, src, dst, target):
        return remote(src, dst, send.at[index], recv.at[index], target)

    def standardize(s):
        step = 64
        for r in range(0, voxels, step):
            values = raw[s, r : r + step, :].astype(jnp.float32)
            center = values - jnp.mean(values, axis=-1, keepdims=True)
            spread = jnp.mean(center * center, axis=-1, keepdims=True)
            result = (center * lax.rsqrt(spread + 1e-05)).astype(jnp.bfloat16)
            zown[2 * s, r : r + step, :] = result[:, :width]
            zown[2 * s + 1, r : r + step, :] = result[:, width:]

    with jax.named_scope("zscore"):
        loads[0].wait()
        standardize(0)
        with jax.named_scope("barrier"):
            pl.semaphore_wait(barrier, len(targets))
        first_on = single(0, zown.at[0:2], zahead.at[0:2], following)
        first_on.start()
        for load in small:
            load.wait()
        near_copy = single(3, near, near_next, previous)
        near_copy.start()
        turn = passed // 2
        for s in order[1 : subjects - turn + 1]:
            loads[s].wait()
            standardize(s)
        back_copy = single(2, zown.at[passed:halves], zback, previous)
        back_copy.start()
        for s in order[subjects - turn + 1 :]:
            loads[s].wait()
            standardize(s)
        rest_on = single(1, zown.at[2:passed], zahead.at[2:passed], following)
        rest_on.start()

    def products(left, right, first, last, left_first=0, right_first=0):
        total = None
        for h in range(first, last):
            term = matmul(left[left_first + h], right[right_first + h], NT)
            total = term if total is None else total + term
        return total

    tile = lax.broadcasted_iota(jnp.int32, (8, voxels), 0)

    def slots_of(ref):
        return [jnp.broadcast_to(ref[k : k + 1, :], (8, voxels)) for k in range(offsets)]

    def picked(source, slots, first, last, sums):
        def body(r, sums):
            ids = tile + r * 8
            values = source[pl.ds(pl.multiple_of(r * 8, 8), 8), :]
            return tuple(
                total + jnp.where(ids == slots[k], values, 0.0)
                for k, total in enumerate(sums)
            )

        return lax.fori_loop(first // 8, last // 8, body, sums, unroll=2)

    def down(sums, target):
        for k in range(offsets):
            target[k : k + 1, :] = jnp.sum(sums[k], axis=0, keepdims=True)

    nothing = tuple(jnp.zeros((8, voxels), jnp.float32) for _ in range(offsets))
    with jax.named_scope("pick_own"):
        corr[voxels:, :] = products(zown, zown, 0, halves)
        sums = picked(corr, slots_of(near), voxels, 2 * voxels, nothing)
        down(sums, part)
        vectors = live[...].astype(jnp.float32) * begin[...]
        halo_out[0] = vectors
    with jax.named_scope("wait_first"):
        first_on.wait_recv()
    corr[:voxels, :] = products(zahead, zown, 0, 2)
    with jax.named_scope("wait_back"):
        near_copy.wait_recv()
        back_copy.wait_recv()
    with jax.named_scope("pick_next"):
        corr_next[...] = products(zown, zback, 0, halves - passed, left_first=passed)
        down(picked(corr_next, slots_of(near_next), 0, voxels, nothing), part_next)
    next_copy = single(4, part_next, part_in, following)
    next_copy.start()
    with jax.named_scope("wait_rest"):
        rest_on.wait_recv()
    with jax.named_scope("pick_cross"):
        corr[:voxels, :] += products(zahead, zown, 2, passed)
        down(picked(corr, slots_of(near), 0, voxels, sums), part)
    with jax.named_scope("wait_part"):
        next_copy.wait_recv()
    part[...] += part_in[...]

    part_copies = []
    for d, peer in enumerate(group_peers):
        copy = remote(
            part, parts.at[group], part_send.at[d], part_recv.at[group], {"subj": peer}
        )
        copy.start()
        part_copies.append(copy)

    def halo(t):
        return (
            remote(halo_out.at[t], from_prev.at[t], halo_send.at[t, 0], halo_recv.at[t, 0], following),
            remote(halo_out.at[t], from_next.at[t], halo_send.at[t, 1], halo_recv.at[t, 1], previous),
        )

    for copy in halo(0):
        copy.start()
    parts[group] = part[...]
    with jax.named_scope("subj_wait"):
        for d, peer in enumerate(group_peers):
            remote(
                part, parts.at[peer], part_send.at[d], part_recv.at[peer], {"subj": peer}
            ).wait_recv()
    summed = parts[0]
    for g in range(1, groups):
        summed = summed + parts[g]
    weight = jnp.where(near[...] >= 0, jnp.exp(scale_factor * summed), 0.0)
    listed[...] = weight
    list_copy = single(5, listed, listed_next, previous)
    list_copy.start()

    def dense(near_table, weight_table, high_out, low_out, rows_total):
        slots, weights = slots_of(near_table), slots_of(weight_table)

        @pl.loop(0, rows_total // 16)
        def _(r):
            tiles = []
            for h in range(2):
                ids = tile + (r * 16 + h * 8)
                entry = jnp.zeros((8, voxels), jnp.float32)
                for k in range(offsets):
                    entry = jnp.where(ids == slots[k], weights[k], entry)
                tiles.append(entry)
            high, low = split(jnp.concatenate(tiles, axis=0))
            rows = pl.ds(pl.multiple_of(r * 16, 16), 16)
            high_out[rows, :] = high
            low_out[rows, :] = low

    ones = jnp.ones((8, voxels), jnp.bfloat16)
    with jax.named_scope("dense"):
        dense(near, listed, ghigh, glow, 2 * voxels)
        owed = matmul(ones, ghigh[voxels:, :], NT) + matmul(ones, glow[voxels:, :], NT)
    with jax.named_scope("wait_list"):
        list_copy.wait_recv()
    with jax.named_scope("degree"):
        dense(near_next, listed_next, nhigh, nlow, voxels)
        owed = owed + (matmul(ones, nhigh[...], NT) + matmul(ones, nlow[...], NT))
        degree = 1.0 + jnp.sum(listed[...], axis=0, keepdims=True) + owed[:1, :]
        scale_row[...] = live[...].astype(jnp.float32) * lax.rsqrt(degree)
    scale_copies = [
        single(6, scale_row, scale_prev, following),
        single(7, scale_row, scale_next, previous),
    ]
    for copy in scale_copies:
        copy.start()

    def stacked(values):
        high, low = split(values)
        return high, jnp.concatenate([high, low], axis=0)

    def own_part(current):
        scaled = scale_row[...] * current
        high, both = stacked(scaled)
        mine = matmul(both, ghigh[voxels:, :], NT) + matmul(both, ghigh[voxels:, :], NN)
        rest = matmul(high, glow[voxels:, :], NT) + matmul(high, glow[voxels:, :], NN)
        return scaled + (mine[:vecs] + mine[vecs:] + rest)

    def whole_part(current, own, before, after):
        high, both = stacked(before)
        mine = matmul(both, ghigh[:voxels, :], NN)
        rest = matmul(high, glow[:voxels, :], NN)
        high, both = stacked(after)
        mine = mine + matmul(both, nhigh[...], NT)
        rest = rest + matmul(high, nlow[...], NT)
        total = own + (mine[:vecs] + mine[vecs:] + rest)
        return 0.5 * (current + scale_row[...] * total)

    own = own_part(vectors)
    with jax.named_scope("wait_scale"):
        for copy in scale_copies + list(halo(0)):
            copy.wait_recv()
    images = whole_part(
        vectors, own, scale_prev[...] * from_prev[0], scale_next[...] * from_next[0]
    )

    lane = lax.broadcasted_iota(jnp.int32, (vecs // 2, 2 * vecs), 1)
    row_all = lax.broadcasted_iota(jnp.int32, (vecs, 2 * vecs), 0)
    lane_all = lax.broadcasted_iota(jnp.int32, (vecs, 2 * vecs), 1)
    identity = (lane_all - vecs == row_all).astype(jnp.float32)
    quarter = vecs // 4

    def send_halo(t, current):
        halo_out[t] = scale_row[...] * current
        for copy in halo(t):
            copy.start()

    def next_images(t, current):
        own = own_part(current)
        with jax.named_scope("wait_halo"):
            for copy in halo(t):
                copy.wait_recv()
        return whole_part(current, own, from_prev[t], from_next[t])

    def stage1_copy(t, d, arriving=False):
        peer = plane_peers[d]
        source = gram.at[t, pl.ds(pl.multiple_of(lax.rem(peer, 2) * quarter, quarter), quarter)]
        target = {"vox": level * plane + peer}
        slot = peer if arriving else spot
        return remote(source, stage1.at[t, slot], s1_send.at[t, d], s1_recv.at[t, slot], target)

    def stage2_copy(t, d, arriving=False):
        peer = level_peers[d]
        target = {"vox": peer * plane + spot}
        slot = peer if arriving else level
        return remote(half.at[t], stage2.at[t, slot], s2_send.at[t, d], s2_recv.at[t, slot], target)

    def stage3_copy(t):
        return remote(whole.at[t], other.at[t], s3_sems.at[t, 0], s3_sems.at[t, 1], partner)

    def sum_start(t, current):
        twice = jnp.concatenate([current, current], axis=0)
        product = matmul(current, twice, NT, HIGHEST)
        gram[t] = jnp.where(lane < vecs, product[: vecs // 2], product[vecs // 2 :])
        for d in range(plane - 1):
            stage1_copy(t, d).start()
        own_rows = pl.ds(pl.multiple_of(core * quarter, quarter), quarter)
        stage1[t, spot] = gram[t, own_rows]

    def sum_planes(t):
        with jax.named_scope(f"s1_wait{t}"):
            for d in range(plane - 1):
                stage1_copy(t, d, True).wait_recv()
        total = stage1[t, 0]
        for p in range(1, plane):
            total = total + stage1[t, p]
        half[t] = total
        for d in range(planes - 1):
            stage2_copy(t, d).start()
        stage2[t, level] = total

    def sum_levels(t):
        with jax.named_scope(f"s2_wait{t}"):
            for d in range(planes - 1):
                stage2_copy(t, d, True).wait_recv()
        total = stage2[t, 0]
        for p in range(1, planes):
            total = total + stage2[t, p]
        whole[t] = total
        stage3_copy(t).start()

    def sum_end(t):
        with jax.named_scope(f"s3_wait{t}"):
            stage3_copy(t).wait_recv()
        total, got = whole[t], other[t]
        upper = jnp.where(core == 0, total, got)
        lower = jnp.where(core == 0, got, total)
        full = jnp.concatenate([upper, lower], axis=0)
        return jnp.concatenate([full, pltpu.roll(full, vecs, 1)], axis=0)

    def inverse_factor(matrix):
        solved = factor_inverse(jnp.where(lane_all < vecs, matrix, identity))
        return pltpu.roll(solved, vecs, 1)[:, :vecs]

    def normalized(inverse, matrix):
        left = matmul(inverse, matrix[:, :vecs], NN, HIGHEST)
        padded = jnp.concatenate([inverse, jnp.zeros_like(inverse)], axis=0)
        return matmul(left, padded, NT, HIGHEST)

    sum_start(0, images)
    send_halo(1, images)
    sum_planes(0)
    images = next_images(1, images)
    sum_start(1, images)
    sum_levels(0)
    sum_planes(1)
    matrix = sum_end(0)
    with jax.named_scope("chol0"):
        inverse = inverse_factor(matrix)
    images = matmul(inverse, images, NN, HIGHEST)
    send_halo(2, images)
    images = next_images(2, images)
    sum_start(2, images)
    sum_levels(1)
    sum_planes(2)
    matrix = sum_end(1)
    with jax.named_scope("chol1"):
        inverse = inverse_factor(normalized(inverse, matrix))
    images = matmul(inverse, images, NN, HIGHEST)
    sum_levels(2)
    matrix = sum_end(2)
    with jax.named_scope("chol2"):
        inverse = inverse_factor(normalized(inverse, matrix))
    out_ref[...] = matmul(inverse, images, NN, HIGHEST)

    with jax.named_scope("tail"):
        singles = [first_on, rest_on, back_copy, near_copy, next_copy, list_copy]
        for copy in singles + scale_copies + part_copies:
            copy.wait_send()
        for t in range(ITERS):
            for copy in halo(t):
                copy.wait_send()
            for d in range(plane - 1):
                stage1_copy(t, d).wait_send()
            for d in range(planes - 1):
                stage2_copy(t, d).wait_send()
            stage3_copy(t).wait_send()


def solution(mesh):
    count, groups = mesh.shape["vox"], mesh.shape["subj"]
    plane = 8 if count >= 16 else count // 2
    planes = count // plane

    def on_device(series, live_mask, neighbours, start_vectors):
        subjects, voxels, frames = series.shape
        vecs = start_vectors.shape[1]
        offsets = neighbours.shape[1]
        scale_factor = 0.5 / math.sqrt(frames * subjects * groups)
        f32, bf16, i32 = jnp.float32, jnp.bfloat16, jnp.int32
        block = (vecs, voxels)
        table = (offsets, voxels)
        line = (1, voxels)
        quarter = (vecs // 4, 2 * vecs)
        halves, width = 2 * subjects, frames // 2
        passed = halves * 5 // 8
        dma = pltpu.SemaphoreType.DMA
        anywhere = pl.BlockSpec(memory_space=pl.ANY)
        result = pl.pallas_call(
            functools.partial(kernel, (groups, plane, planes, scale_factor)),
            out_shape=jax.ShapeDtypeStruct(block, f32),
            in_specs=[anywhere] * 4,
            out_specs=pl.BlockSpec(memory_space=pltpu.VMEM),
            scratch_shapes=[
                pltpu.VMEM((subjects, voxels, frames), bf16),
                pltpu.VMEM((halves, voxels, width), bf16),
                pltpu.VMEM((passed, voxels, width), bf16),
                pltpu.VMEM((halves - passed, voxels, width), bf16),
                pltpu.VMEM(table, i32),
                pltpu.VMEM(table, i32),
                pltpu.VMEM(line, i32),
                pltpu.VMEM(block, f32),
                pltpu.VMEM((2 * voxels, voxels), f32),
                pltpu.VMEM((voxels, voxels), f32),
                pltpu.VMEM(table, f32),
                pltpu.VMEM(table, f32),
                pltpu.VMEM(table, f32),
                pltpu.VMEM((groups, *table), f32),
                pltpu.VMEM(table, f32),
                pltpu.VMEM(table, f32),
                pltpu.VMEM((2 * voxels, voxels), bf16),
                pltpu.VMEM((2 * voxels, voxels), bf16),
                pltpu.VMEM((voxels, voxels), bf16),
                pltpu.VMEM((voxels, voxels), bf16),
                pltpu.VMEM(line, f32),
                pltpu.VMEM(line, f32),
                pltpu.VMEM(line, f32),
                pltpu.VMEM((ITERS, *block), f32),
                pltpu.VMEM((ITERS, *block), f32),
                pltpu.VMEM((ITERS, *block), f32),
                pltpu.VMEM((ITERS, vecs // 2, 2 * vecs), f32),
                pltpu.VMEM((ITERS, plane, *quarter), f32),
                pltpu.VMEM((ITERS, *quarter), f32),
                pltpu.VMEM((ITERS, planes, *quarter), f32),
                pltpu.VMEM((ITERS, *quarter), f32),
                pltpu.VMEM((ITERS, *quarter), f32),
                dma((subjects + 3,)),
                dma((8,)),
                dma((8,)),
                dma((max(groups - 1, 1),)),
                dma((groups,)),
                dma((ITERS, 2)),
                dma((ITERS, 2)),
                dma((ITERS, plane - 1)),
                dma((ITERS, plane)),
                dma((ITERS, planes - 1)),
                dma((ITERS, planes)),
                dma((ITERS, 2)),
            ],
            compiler_params=pltpu.CompilerParams(
                collective_id=0, has_side_effects=True
            ),
        )(series, live_mask.reshape(1, voxels), neighbours.T, start_vectors.T)
        return result.T

    placed = (P("subj", "vox", None), P("vox"), P("vox", None), P("vox", None))
    return jax.shard_map(
        on_device, mesh=mesh, in_specs=placed, out_specs=P("vox", None), check_vma=False
    )
```

```python
import functools
import math

import jax
import jax.numpy as jnp
from jax import lax
from jax.experimental import pallas as pl
from jax.experimental.pallas import tpu as pltpu
from jax.sharding import PartitionSpec as P

ITERS = 3
HIGHEST = lax.Precision.HIGHEST
NN = (((1,), (0,)), ((), ()))
NT = (((1,), (1,)), ((), ()))


def matmul(left, right, dims, precision=None):
    return lax.dot_general(
        left, right, dims, precision=precision, preferred_element_type=jnp.float32
    )


def split(values):
    high = values.astype(jnp.bfloat16)
    low = (values - high.astype(jnp.float32)).astype(jnp.bfloat16)
    return high, low


def factor_inverse(rows):
    total, width = rows.shape
    sublane = lax.broadcasted_iota(jnp.int32, (8, width), 0)
    done = []
    for first in range(0, total, 8):
        left = total - first
        cols = [
            jnp.broadcast_to(rows[:, first + c : first + c + 1], (left, width))
            for c in range(8)
        ]
        block = jnp.zeros((8, width), jnp.float32)
        for c in range(8):
            root = lax.rsqrt(cols[c][c : c + 1, :])
            lower = cols[c] * root
            pivot = rows[c : c + 1, :] * root
            block = jnp.where(sublane == c, pivot, block)
            rows = rows - lower * pivot
            for other in range(c + 1, 8):
                cols[other] = cols[other] - lower * lower[other : other + 1, :]
        done.append(block)
        rows = rows[8:]
    return jnp.concatenate(done, axis=0)


def kernel(
    sizes,
    series_ref,
    mask_ref,
    near_ref,
    start_ref,
    out_ref,
    raw,
    zown,
    zahead,
    zback,
    near,
    near_next,
    live,
    begin,
    corr,
    corr_next,
    part_next,
    part_in,
    part,
    parts,
    listed,
    listed_next,
    ghigh,
    glow,
    nhigh,
    nlow,
    scale_row,
    shares,
    shares_prev,
    shares_next,
    shares_second,
    halo_out,
    from_prev,
    from_next,
    gram,
    stage1,
    half,
    stage2,
    in_sems,
    send,
    recv,
    part_send,
    part_recv,
    halo_send,
    halo_recv,
    s1_send,
    s1_recv,
    s2_send,
    s2_recv,
):
    groups, plane, planes, scale_factor = sizes
    count = plane * planes
    subjects, voxels, frames = series_ref.shape
    offsets = near_ref.shape[0]
    vecs = start_ref.shape[0]
    halves, width = 2 * subjects, frames // 2
    passed = zahead.shape[0]
    me = lax.axis_index("vox")
    group = lax.axis_index("subj")
    spot = lax.rem(me, plane)
    level = me // plane
    following = {"vox": lax.rem(me + 1, count)}
    previous = {"vox": lax.rem(me + count - 1, count)}
    second = {"vox": lax.rem(me + count - 2, count)}

    plane_peers = [lax.rem(spot + d, plane) for d in range(1, plane)]
    level_peers = [lax.rem(level + d, planes) for d in range(1, planes)]
    group_peers = [lax.rem(group + d, groups) for d in range(1, groups)]

    loads = [
        pltpu.make_async_copy(series_ref.at[s], raw.at[s], in_sems.at[s])
        for s in range(subjects)
    ]
    small = [
        pltpu.make_async_copy(near_ref, near, in_sems.at[subjects]),
        pltpu.make_async_copy(mask_ref, live, in_sems.at[subjects + 1]),
        pltpu.make_async_copy(start_ref, begin, in_sems.at[subjects + 2]),
    ]
    for load in loads + small:
        load.start()

    barrier = pltpu.get_barrier_semaphore()
    targets = [following, previous, {"vox": lax.rem(me + 2, count)}, second]
    targets += [{"vox": level * plane + p} for p in plane_peers]
    targets += [{"vox": p * plane + spot} for p in level_peers]
    targets += [{"subj": p} for p in group_peers]
    for target in targets:
        pl.semaphore_signal(
            barrier, inc=1, device_id=target, device_id_type=pl.DeviceIdType.MESH
        )

    def remote(src, dst, send_sem, recv_sem, target):
        return pltpu.make_async_remote_copy(
            src_ref=src,
            dst_ref=dst,
            send_sem=send_sem,
            recv_sem=recv_sem,
            device_id=target,
            device_id_type=pl.DeviceIdType.MESH,
        )

    def single(index, src, dst, target):
        return remote(src, dst, send.at[index], recv.at[index], target)

    def standardize(s):
        step = 64
        for r in range(0, voxels, step):
            values = raw[s, r : r + step, :].astype(jnp.float32)
            center = values - jnp.mean(values, axis=-1, keepdims=True)
            spread = jnp.mean(center * center, axis=-1, keepdims=True)
            result = (center * lax.rsqrt(spread + 1e-05)).astype(jnp.bfloat16)
            zown[2 * s, r : r + step, :] = result[:, :width]
            zown[2 * s + 1, r : r + step, :] = result[:, width:]

    with jax.named_scope("zscore"):
        for s in range(subjects):
            loads[s].wait()
            standardize(s)
        for load in small:
            load.wait()
    with jax.named_scope("barrier"):
        pl.semaphore_wait(barrier, len(targets))
    back_copy = single(2, zown.at[passed:halves], zback, previous)
    first_on = single(0, zown.at[0:2], zahead.at[0:2], following)
    rest_on = single(1, zown.at[2:passed], zahead.at[2:passed], following)
    near_copy = single(3, near, near_next, previous)
    for copy in (near_copy, back_copy, first_on, rest_on):
        copy.start()

    def products(left, right, first, last, left_first=0, right_first=0):
        total = None
        for h in range(first, last):
            term = matmul(left[left_first + h], right[right_first + h], NT)
            total = term if total is None else total + term
        return total

    tile = lax.broadcasted_iota(jnp.int32, (8, voxels), 0)

    def slots_of(ref):
        return [jnp.broadcast_to(ref[k : k + 1, :], (8, voxels)) for k in range(offsets)]

    def picked(source, slots, first, last, sums):
        def body(r, sums):
            ids = tile + r * 8
            values = source[pl.ds(pl.multiple_of(r * 8, 8), 8), :]
            return tuple(
                total + jnp.where(ids == slots[k], values, 0.0)
                for k, total in enumerate(sums)
            )

        return lax.fori_loop(first // 8, last // 8, body, sums, unroll=2)

    def down(sums, target):
        for k in range(offsets):
            target[k : k + 1, :] = jnp.sum(sums[k], axis=0, keepdims=True)

    nothing = tuple(jnp.zeros((8, voxels), jnp.float32) for _ in range(offsets))
    with jax.named_scope("pick_own"):
        corr[voxels:, :] = products(zown, zown, 0, halves)
        sums = picked(corr, slots_of(near), voxels, 2 * voxels, nothing)
        down(sums, part)
        vectors = live[...].astype(jnp.float32) * begin[...]
        halo_out[0] = vectors
    with jax.named_scope("wait_first"):
        first_on.wait_recv()
    corr[:voxels, :] = products(zahead, zown, 0, 2)
    with jax.named_scope("wait_back"):
        near_copy.wait_recv()
        back_copy.wait_recv()
    with jax.named_scope("pick_next"):
        corr_next[...] = products(zown, zback, 0, halves - passed, left_first=passed)
        down(picked(corr_next, slots_of(near_next), 0, voxels, nothing), part_next)
    next_copy = single(4, part_next, part_in, following)
    next_copy.start()
    with jax.named_scope("wait_rest"):
        rest_on.wait_recv()
    with jax.named_scope("pick_cross"):
        corr[:voxels, :] += products(zahead, zown, 2, passed)
        down(picked(corr, slots_of(near), 0, voxels, sums), part)
    with jax.named_scope("wait_part"):
        next_copy.wait_recv()
    part[...] += part_in[...]

    part_copies = []
    for d, peer in enumerate(group_peers):
        copy = remote(
            part, parts.at[group], part_send.at[d], part_recv.at[group], {"subj": peer}
        )
        copy.start()
        part_copies.append(copy)

    def halo(t):
        return (
            remote(halo_out.at[t], from_prev.at[t], halo_send.at[t, 0], halo_recv.at[t, 0], following),
            remote(halo_out.at[t], from_next.at[t], halo_send.at[t, 1], halo_recv.at[t, 1], previous),
        )

    for copy in halo(0):
        copy.start()
    parts[group] = part[...]
    with jax.named_scope("subj_wait"):
        for d, peer in enumerate(group_peers):
            remote(
                part, parts.at[peer], part_send.at[d], part_recv.at[peer], {"subj": peer}
            ).wait_recv()
    summed = parts[0]
    for g in range(1, groups):
        summed = summed + parts[g]
    weight = jnp.where(near[...] >= 0, jnp.exp(scale_factor * summed), 0.0)
    listed[...] = weight
    list_copy = single(5, listed, listed_next, previous)
    list_copy.start()

    def dense(near_table, weight_table, high_out, low_out, rows_total):
        slots, weights = slots_of(near_table), slots_of(weight_table)

        @pl.loop(0, rows_total // 16)
        def _(r):
            tiles = []
            for h in range(2):
                ids = tile + (r * 16 + h * 8)
                entry = jnp.zeros((8, voxels), jnp.float32)
                for k in range(offsets):
                    entry = jnp.where(ids == slots[k], weights[k], entry)
                tiles.append(entry)
            high, low = split(jnp.concatenate(tiles, axis=0))
            rows = pl.ds(pl.multiple_of(r * 16, 16), 16)
            high_out[rows, :] = high
            low_out[rows, :] = low

    ones = jnp.ones((8, voxels), jnp.bfloat16)
    with jax.named_scope("dense"):
        dense(near, listed, ghigh, glow, 2 * voxels)
        owed = matmul(ones, ghigh[...], NT) + matmul(ones, glow[...], NT)
        shares[:1, :] = (
            1.0 + jnp.sum(listed[...], axis=0, keepdims=True) + owed[:1, voxels:]
        )
        shares[1:2, :] = owed[:1, :voxels]
    share_copies = [
        single(6, shares, shares_prev, following),
        single(7, shares, shares_next, previous),
        single(8, shares, shares_second, second),
    ]
    for copy in share_copies:
        copy.start()
    with jax.named_scope("wait_list"):
        list_copy.wait_recv()
    with jax.named_scope("dense_next"):
        dense(near_next, listed_next, nhigh, nlow, voxels)

    def stacked(values):
        high, low = split(values)
        return high, jnp.concatenate([high, low], axis=0)

    def own_part(current):
        scaled = scale_row[...] * current
        high, both = stacked(scaled)
        mine = matmul(both, ghigh[voxels:, :], NT) + matmul(both, ghigh[voxels:, :], NN)
        rest = matmul(high, glow[voxels:, :], NT) + matmul(high, glow[voxels:, :], NN)
        return scaled + (mine[:vecs] + mine[vecs:] + rest)

    def whole_part(current, own, before, after):
        high, both = stacked(before)
        mine = matmul(both, ghigh[:voxels, :], NN)
        rest = matmul(high, glow[:voxels, :], NN)
        high, both = stacked(after)
        mine = mine + matmul(both, nhigh[...], NT)
        rest = rest + matmul(high, nlow[...], NT)
        total = own + (mine[:vecs] + mine[vecs:] + rest)
        return 0.5 * (current + scale_row[...] * total)

    with jax.named_scope("wait_shares"):
        for copy in share_copies + list(halo(0)):
            copy.wait_recv()
    with jax.named_scope("images0"):
        scale_row[...] = live[...].astype(jnp.float32) * lax.rsqrt(
            shares[:1, :] + shares_next[1:2, :]
        )
        scale_prev = lax.rsqrt(shares_prev[:1, :] + shares[1:2, :])
        scale_next = lax.rsqrt(shares_next[:1, :] + shares_second[1:2, :])
        images = whole_part(
            vectors, own_part(vectors), scale_prev * from_prev[0], scale_next * from_next[0]
        )

    mid = vecs // 2
    lane = lax.broadcasted_iota(jnp.int32, (mid, 2 * vecs), 1)
    row = lax.broadcasted_iota(jnp.int32, (mid, 2 * vecs), 0)
    column = lax.rem(lane, vecs)
    row_all = lax.broadcasted_iota(jnp.int32, (vecs, 2 * vecs), 0)
    lane_all = lax.broadcasted_iota(jnp.int32, (vecs, 2 * vecs), 1)
    identity = (lane_all - vecs == row_all).astype(jnp.float32)
    fold = mid // 2

    def send_halo(t, current):
        halo_out[t] = scale_row[...] * current
        for copy in halo(t):
            copy.start()

    def next_images(t, current):
        own = own_part(current)
        with jax.named_scope("wait_halo"):
            for copy in halo(t):
                copy.wait_recv()
        return whole_part(current, own, from_prev[t], from_next[t])

    def stage1_copy(t, d, arriving=False):
        peer = plane_peers[d]
        target = {"vox": level * plane + peer}
        slot = peer if arriving else spot
        return remote(gram.at[t], stage1.at[t, slot], s1_send.at[t, d], s1_recv.at[t, slot], target)

    def stage2_copy(t, d, arriving=False):
        peer = level_peers[d]
        target = {"vox": peer * plane + spot}
        slot = peer if arriving else level
        return remote(half.at[t], stage2.at[t, slot], s2_send.at[t, d], s2_recv.at[t, slot], target)

    def sum_start(t, current):
        upper, lower = current[:mid], current[mid:]
        first = matmul(upper, jnp.concatenate([upper, lower] * 2, axis=0), NT, HIGHEST)
        last = matmul(lower, jnp.concatenate([lower] * 4, axis=0), NT, HIGHEST)
        square = jnp.where((column < mid) & (row < column), last, first)
        gram[t, : fold, :] = jnp.where(lane[:fold] < vecs, square[:fold], square[fold:])
        gram[t, fold : fold + 1, :] = jnp.sum(
            jnp.where(row == column, last, 0.0), axis=0, keepdims=True
        )
        for d in range(plane - 1):
            stage1_copy(t, d).start()
        stage1[t, spot] = gram[t]

    def sum_planes(t):
        with jax.named_scope(f"s1_wait{t}"):
            for d in range(plane - 1):
                stage1_copy(t, d, True).wait_recv()
        total = stage1[t, 0]
        for p in range(1, plane):
            total = total + stage1[t, p]
        half[t] = total
        for d in range(planes - 1):
            stage2_copy(t, d).start()
        stage2[t, level] = total

    def sum_end(t):
        with jax.named_scope(f"s2_wait{t}"):
            for d in range(planes - 1):
                stage2_copy(t, d, True).wait_recv()
        total = stage2[t, 0]
        for p in range(1, planes):
            total = total + stage2[t, p]
        folded, diagonal = total[:fold], total[fold : fold + 1]
        square = jnp.concatenate([folded, pltpu.roll(folded, vecs, 1)], axis=0)
        filled = jnp.concatenate(
            [square, jnp.zeros((2 * vecs - mid, 2 * vecs), jnp.float32)], axis=0
        )
        turned = filled.T
        top = jnp.where((lane < mid) & (row < lane), turned[:mid], square)
        corner = jnp.where(row < lane, square, jnp.where(row == lane, diagonal, turned[:mid]))
        bottom = jnp.where(lane < mid, turned[mid:vecs], pltpu.roll(corner, mid, 1))
        return jnp.concatenate([top, bottom], axis=0)

    def inverse_factor(matrix):
        solved = factor_inverse(jnp.where(lane_all < vecs, matrix, identity))
        return pltpu.roll(solved, vecs, 1)[:, :vecs]

    def normalized(inverse, matrix):
        left = matmul(inverse, matrix[:, :vecs], NN, HIGHEST)
        padded = jnp.concatenate([inverse, jnp.zeros_like(inverse)], axis=0)
        return matmul(left, padded, NT, HIGHEST)

    sum_start(0, images)
    send_halo(1, images)
    sum_planes(0)
    images = next_images(1, images)
    sum_start(1, images)
    matrix = sum_end(0)
    sum_planes(1)
    with jax.named_scope("chol0"):
        inverse = inverse_factor(matrix)
    images = matmul(inverse, images, NN, HIGHEST)
    send_halo(2, images)
    images = next_images(2, images)
    sum_start(2, images)
    matrix = sum_end(1)
    sum_planes(2)
    with jax.named_scope("chol1"):
        inverse = inverse_factor(normalized(inverse, matrix))
    images = matmul(inverse, images, NN, HIGHEST)
    matrix = sum_end(2)
    with jax.named_scope("chol2"):
        inverse = inverse_factor(normalized(inverse, matrix))
    out_ref[...] = matmul(inverse, images, NN, HIGHEST)

    with jax.named_scope("tail"):
        singles = [first_on, rest_on, back_copy, near_copy, next_copy, list_copy]
        for copy in singles + share_copies + part_copies:
            copy.wait_send()
        for t in range(ITERS):
            for copy in halo(t):
                copy.wait_send()
            for d in range(plane - 1):
                stage1_copy(t, d).wait_send()
            for d in range(planes - 1):
                stage2_copy(t, d).wait_send()


def solution(mesh):
    count, groups = mesh.shape["vox"], mesh.shape["subj"]
    plane = 8 if count >= 16 else count // 2
    planes = count // plane

    def on_device(series, live_mask, neighbours, start_vectors):
        subjects, voxels, frames = series.shape
        vecs = start_vectors.shape[1]
        offsets = neighbours.shape[1]
        scale_factor = 0.5 / math.sqrt(frames * subjects * groups)
        f32, bf16, i32 = jnp.float32, jnp.bfloat16, jnp.int32
        block = (vecs, voxels)
        table = (offsets, voxels)
        line = (1, voxels)
        packed = (vecs // 4 + 1, 2 * vecs)
        halves, width = 2 * subjects, frames // 2
        passed = halves * 3 // 4
        dma = pltpu.SemaphoreType.DMA
        outside = pl.BlockSpec(memory_space=pltpu.HBM)
        result = pl.pallas_call(
            functools.partial(kernel, (groups, plane, planes, scale_factor)),
            out_shape=jax.ShapeDtypeStruct(block, f32),
            in_specs=[outside] * 4,
            out_specs=pl.BlockSpec(memory_space=pltpu.VMEM),
            scratch_shapes=[
                pltpu.VMEM((subjects, voxels, frames), bf16),
                pltpu.VMEM((halves, voxels, width), bf16),
                pltpu.VMEM((passed, voxels, width), bf16),
                pltpu.VMEM((halves - passed, voxels, width), bf16),
                pltpu.VMEM(table, i32),
                pltpu.VMEM(table, i32),
                pltpu.VMEM(line, i32),
                pltpu.VMEM(block, f32),
                pltpu.VMEM((2 * voxels, voxels), f32),
                pltpu.VMEM((voxels, voxels), f32),
                pltpu.VMEM(table, f32),
                pltpu.VMEM(table, f32),
                pltpu.VMEM(table, f32),
                pltpu.VMEM((groups, *table), f32),
                pltpu.VMEM(table, f32),
                pltpu.VMEM(table, f32),
                pltpu.VMEM((2 * voxels, voxels), bf16),
                pltpu.VMEM((2 * voxels, voxels), bf16),
                pltpu.VMEM((voxels, voxels), bf16),
                pltpu.VMEM((voxels, voxels), bf16),
                pltpu.VMEM(line, f32),
                pltpu.VMEM((2, voxels), f32),
                pltpu.VMEM((2, voxels), f32),
                pltpu.VMEM((2, voxels), f32),
                pltpu.VMEM((2, voxels), f32),
                pltpu.VMEM((ITERS, *block), f32),
                pltpu.VMEM((ITERS, *block), f32),
                pltpu.VMEM((ITERS, *block), f32),
                pltpu.VMEM((ITERS, *packed), f32),
                pltpu.VMEM((ITERS, plane, *packed), f32),
                pltpu.VMEM((ITERS, *packed), f32),
                pltpu.VMEM((ITERS, planes, *packed), f32),
                dma((subjects + 3,)),
                dma((9,)),
                dma((9,)),
                dma((max(groups - 1, 1),)),
                dma((groups,)),
                dma((ITERS, 2)),
                dma((ITERS, 2)),
                dma((ITERS, plane - 1)),
                dma((ITERS, plane)),
                dma((ITERS, planes - 1)),
                dma((ITERS, planes)),
            ],
            compiler_params=pltpu.CompilerParams(
                collective_id=0, has_side_effects=True, vmem_limit_bytes=32 << 20
            ),
        )(
            *(
                pltpu.with_memory_space_constraint(operand, pltpu.HBM)
                for operand in (
                    series, live_mask.reshape(1, voxels), neighbours.T, start_vectors.T
                )
            )
        )
        return result.T

    placed = (P("subj", "vox", None), P("vox"), P("vox", None), P("vox", None))
    return jax.shard_map(
        on_device, mesh=mesh, in_specs=placed, out_specs=P("vox", None), check_vma=False
    )
```

```python
import functools
import math

import jax
import jax.numpy as jnp
from jax import lax
from jax.experimental import pallas as pl
from jax.experimental.pallas import tpu as pltpu
from jax.sharding import PartitionSpec as P

ITERS = 3
HIGHEST = lax.Precision.HIGHEST
NN = (((1,), (0,)), ((), ()))
NT = (((1,), (1,)), ((), ()))


def matmul(left, right, dims, precision=None):
    return lax.dot_general(
        left, right, dims, precision=precision, preferred_element_type=jnp.float32
    )


def split(values):
    high = values.astype(jnp.bfloat16)
    low = (values - high.astype(jnp.float32)).astype(jnp.bfloat16)
    return high, low


def factor_inverse(rows):
    total, width = rows.shape
    sublane = lax.broadcasted_iota(jnp.int32, (8, width), 0)
    done = []
    for first in range(0, total, 8):
        left = total - first
        cols = [
            jnp.broadcast_to(rows[:, first + c : first + c + 1], (left, width))
            for c in range(8)
        ]
        block = jnp.zeros((8, width), jnp.float32)
        for c in range(8):
            root = lax.rsqrt(cols[c][c : c + 1, :])
            lower = cols[c] * root
            pivot = rows[c : c + 1, :] * root
            block = jnp.where(sublane == c, pivot, block)
            rows = rows - lower * pivot
            for other in range(c + 1, 8):
                cols[other] = cols[other] - lower * lower[other : other + 1, :]
        done.append(block)
        rows = rows[8:]
    return jnp.concatenate(done, axis=0)


def kernel(
    sizes,
    series_ref,
    mask_ref,
    near_ref,
    start_ref,
    out_ref,
    raw,
    zown,
    zahead,
    zback,
    near,
    near_next,
    live,
    begin,
    corr,
    corr_next,
    part_next,
    part_in,
    part,
    parts,
    listed,
    listed_next,
    ghigh,
    glow,
    nhigh,
    nlow,
    scale_row,
    shares,
    shares_prev,
    shares_next,
    shares_second,
    halo_out,
    from_prev,
    from_next,
    gram,
    stage1,
    half,
    stage2,
    in_sems,
    send,
    recv,
    part_send,
    part_recv,
    halo_send,
    halo_recv,
    s1_send,
    s1_recv,
    s2_send,
    s2_recv,
):
    groups, plane, planes, scale_factor = sizes
    count = plane * planes
    subjects, voxels, frames = series_ref.shape
    offsets = near_ref.shape[0]
    vecs = start_ref.shape[0]
    halves, width = 2 * subjects, frames // 2
    passed = zahead.shape[0]
    me = lax.axis_index("vox")
    group = lax.axis_index("subj")
    core = lax.rem(me, 2)
    spot = lax.rem(me, plane)
    level = me // plane
    following = {"vox": lax.rem(me + 1, count)}
    previous = {"vox": lax.rem(me + count - 1, count)}
    second = {"vox": lax.rem(me + count - 2, count)}

    plane_peers = [lax.rem(spot + d, plane) for d in range(1, plane)]
    level_peers = [lax.rem(level + d, planes) for d in range(1, planes)]
    group_peers = [lax.rem(group + d, groups) for d in range(1, groups)]

    loads = [
        pltpu.make_async_copy(series_ref.at[s], raw.at[s], in_sems.at[s])
        for s in range(subjects)
    ]
    small = [
        pltpu.make_async_copy(near_ref, near, in_sems.at[subjects]),
        pltpu.make_async_copy(mask_ref, live, in_sems.at[subjects + 1]),
        pltpu.make_async_copy(start_ref, begin, in_sems.at[subjects + 2]),
    ]
    for load in loads + small:
        load.start()

    barrier = pltpu.get_barrier_semaphore()
    targets = [following, previous, {"vox": lax.rem(me + 2, count)}, second]
    targets += [{"vox": level * plane + p} for p in plane_peers]
    targets += [{"vox": p * plane + spot} for p in level_peers]
    targets += [{"subj": p} for p in group_peers]
    for target in targets:
        pl.semaphore_signal(
            barrier, inc=1, device_id=target, device_id_type=pl.DeviceIdType.MESH
        )

    def remote(src, dst, send_sem, recv_sem, target):
        return pltpu.make_async_remote_copy(
            src_ref=src,
            dst_ref=dst,
            send_sem=send_sem,
            recv_sem=recv_sem,
            device_id=target,
            device_id_type=pl.DeviceIdType.MESH,
        )

    def single(index, src, dst, target):
        return remote(src, dst, send.at[index], recv.at[index], target)

    def standardize(s):
        step = 64
        for r in range(0, voxels, step):
            values = raw[s, r : r + step, :].astype(jnp.float32)
            center = values - jnp.mean(values, axis=-1, keepdims=True)
            spread = jnp.mean(center * center, axis=-1, keepdims=True)
            result = (center * lax.rsqrt(spread + 1e-05)).astype(jnp.bfloat16)
            zown[2 * s, r : r + step, :] = result[:, :width]
            zown[2 * s + 1, r : r + step, :] = result[:, width:]

    with jax.named_scope("zscore"):
        for s in range(subjects):
            loads[s].wait()
            standardize(s)
        for load in small:
            load.wait()
    with jax.named_scope("barrier"):
        pl.semaphore_wait(barrier, len(targets))
    back_copy = single(2, zown.at[passed:halves], zback, previous)
    first_on = single(0, zown.at[0:2], zahead.at[0:2], following)
    rest_on = single(1, zown.at[2 : passed - 1], zahead.at[2 : passed - 1], following)
    last_on = single(9, zown.at[passed - 1 : passed], zahead.at[passed - 1 : passed], following)
    near_copy = single(3, near, near_next, previous)
    ons = [first_on, rest_on, last_on]
    backs = [near_copy, back_copy]

    def start_for(parity, copies):
        @pl.when(core == parity)
        def _():
            for copy in copies:
                copy.start()

    start_for(1, ons)
    start_for(0, backs)

    def products(left, right, first, last, left_first=0, right_first=0):
        total = None
        for h in range(first, last):
            term = matmul(left[left_first + h], right[right_first + h], NT)
            total = term if total is None else total + term
        return total

    tile = lax.broadcasted_iota(jnp.int32, (8, voxels), 0)

    def slots_of(ref):
        return [jnp.broadcast_to(ref[k : k + 1, :], (8, voxels)) for k in range(offsets)]

    def picked(source, slots, first, last, sums):
        def body(r, sums):
            ids = tile + r * 8
            values = source[pl.ds(pl.multiple_of(r * 8, 8), 8), :]
            return tuple(
                total + jnp.where(ids == slots[k], values, 0.0)
                for k, total in enumerate(sums)
            )

        return lax.fori_loop(first // 8, last // 8, body, sums, unroll=2)

    def down(sums, target):
        for k in range(offsets):
            target[k : k + 1, :] = jnp.sum(sums[k], axis=0, keepdims=True)

    nothing = tuple(jnp.zeros((8, voxels), jnp.float32) for _ in range(offsets))
    with jax.named_scope("pick_own"):
        corr[voxels:, :] = products(zown, zown, 0, halves)
        sums = picked(corr, slots_of(near), voxels, 2 * voxels, nothing)
        down(sums, part)
        vectors = live[...].astype(jnp.float32) * begin[...]
        halo_out[0] = vectors
    start_for(0, ons)
    start_for(1, backs)
    with jax.named_scope("wait_first"):
        first_on.wait_recv()
    corr[:voxels, :] = products(zahead, zown, 0, 2)
    with jax.named_scope("wait_back"):
        near_copy.wait_recv()
        back_copy.wait_recv()
    with jax.named_scope("pick_next"):
        corr_next[...] = products(zown, zback, 0, halves - passed, left_first=passed)
        down(picked(corr_next, slots_of(near_next), 0, voxels, nothing), part_next)
    next_copy = single(4, part_next, part_in, following)
    next_copy.start()
    with jax.named_scope("wait_rest"):
        rest_on.wait_recv()
    corr[:voxels, :] += products(zahead, zown, 2, passed - 1)
    with jax.named_scope("wait_last"):
        last_on.wait_recv()
    with jax.named_scope("pick_cross"):
        corr[:voxels, :] += products(zahead, zown, passed - 1, passed)
        down(picked(corr, slots_of(near), 0, voxels, sums), part)
    with jax.named_scope("wait_part"):
        next_copy.wait_recv()
    part[...] += part_in[...]

    part_copies = []
    for d, peer in enumerate(group_peers):
        copy = remote(
            part, parts.at[group], part_send.at[d], part_recv.at[group], {"subj": peer}
        )
        copy.start()
        part_copies.append(copy)

    def halo(t):
        return (
            remote(halo_out.at[t], from_prev.at[t], halo_send.at[t, 0], halo_recv.at[t, 0], following),
            remote(halo_out.at[t], from_next.at[t], halo_send.at[t, 1], halo_recv.at[t, 1], previous),
        )

    for copy in halo(0):
        copy.start()
    parts[group] = part[...]
    with jax.named_scope("subj_wait"):
        for d, peer in enumerate(group_peers):
            remote(
                part, parts.at[peer], part_send.at[d], part_recv.at[peer], {"subj": peer}
            ).wait_recv()
    summed = parts[0]
    for g in range(1, groups):
        summed = summed + parts[g]
    weight = jnp.where(near[...] >= 0, jnp.exp(scale_factor * summed), 0.0)
    listed[...] = weight
    list_copy = single(5, listed, listed_next, previous)
    list_copy.start()

    def dense(near_table, weight_table, high_out, low_out, rows_total):
        slots, weights = slots_of(near_table), slots_of(weight_table)

        @pl.loop(0, rows_total // 16)
        def _(r):
            tiles = []
            for h in range(2):
                ids = tile + (r * 16 + h * 8)
                entry = jnp.zeros((8, voxels), jnp.float32)
                for k in range(offsets):
                    entry = jnp.where(ids == slots[k], weights[k], entry)
                tiles.append(entry)
            high, low = split(jnp.concatenate(tiles, axis=0))
            rows = pl.ds(pl.multiple_of(r * 16, 16), 16)
            high_out[rows, :] = high
            low_out[rows, :] = low

    ones = jnp.ones((8, voxels), jnp.bfloat16)
    with jax.named_scope("dense"):
        dense(near, listed, ghigh, glow, 2 * voxels)
        owed = matmul(ones, ghigh[...], NT) + matmul(ones, glow[...], NT)
        shares[:1, :] = (
            1.0 + jnp.sum(listed[...], axis=0, keepdims=True) + owed[:1, voxels:]
        )
        shares[1:2, :] = owed[:1, :voxels]
    share_copies = [
        single(6, shares, shares_prev, following),
        single(7, shares, shares_next, previous),
        single(8, shares, shares_second, second),
    ]
    for copy in share_copies:
        copy.start()
    with jax.named_scope("wait_list"):
        list_copy.wait_recv()
    with jax.named_scope("dense_next"):
        dense(near_next, listed_next, nhigh, nlow, voxels)

    def stacked(values):
        high, low = split(values)
        return high, jnp.concatenate([high, low], axis=0)

    def own_part(current):
        scaled = scale_row[...] * current
        high, both = stacked(scaled)
        mine = matmul(both, ghigh[voxels:, :], NT) + matmul(both, ghigh[voxels:, :], NN)
        rest = matmul(high, glow[voxels:, :], NT) + matmul(high, glow[voxels:, :], NN)
        return scaled + (mine[:vecs] + mine[vecs:] + rest)

    def whole_part(current, own, before, after):
        high, both = stacked(before)
        mine = matmul(both, ghigh[:voxels, :], NN)
        rest = matmul(high, glow[:voxels, :], NN)
        high, both = stacked(after)
        mine = mine + matmul(both, nhigh[...], NT)
        rest = rest + matmul(high, nlow[...], NT)
        total = own + (mine[:vecs] + mine[vecs:] + rest)
        return 0.5 * (current + scale_row[...] * total)

    with jax.named_scope("wait_shares"):
        for copy in share_copies + list(halo(0)):
            copy.wait_recv()
    with jax.named_scope("images0"):
        scale_row[...] = live[...].astype(jnp.float32) * lax.rsqrt(
            shares[:1, :] + shares_next[1:2, :]
        )
        scale_prev = lax.rsqrt(shares_prev[:1, :] + shares[1:2, :])
        scale_next = lax.rsqrt(shares_next[:1, :] + shares_second[1:2, :])
        images = whole_part(
            vectors, own_part(vectors), scale_prev * from_prev[0], scale_next * from_next[0]
        )

    mid = vecs // 2
    lane = lax.broadcasted_iota(jnp.int32, (mid, 2 * vecs), 1)
    row = lax.broadcasted_iota(jnp.int32, (mid, 2 * vecs), 0)
    column = lax.rem(lane, vecs)
    row_all = lax.broadcasted_iota(jnp.int32, (vecs, 2 * vecs), 0)
    lane_all = lax.broadcasted_iota(jnp.int32, (vecs, 2 * vecs), 1)
    identity = (lane_all - vecs == row_all).astype(jnp.float32)
    fold = mid // 2

    def send_halo(t, current):
        halo_out[t] = scale_row[...] * current
        for copy in halo(t):
            copy.start()

    def next_images(t, current, own):
        with jax.named_scope("wait_halo"):
            for copy in halo(t):
                copy.wait_recv()
        return whole_part(current, own, from_prev[t], from_next[t])

    def stage1_copy(t, d, arriving=False):
        peer = plane_peers[d]
        target = {"vox": level * plane + peer}
        slot = peer if arriving else spot
        return remote(gram.at[t], stage1.at[t, slot], s1_send.at[t, d], s1_recv.at[t, slot], target)

    def stage2_copy(t, d, arriving=False):
        peer = level_peers[d]
        target = {"vox": peer * plane + spot}
        slot = peer if arriving else level
        return remote(half.at[t], stage2.at[t, slot], s2_send.at[t, d], s2_recv.at[t, slot], target)

    def sum_start(t, current):
        upper, lower = current[:mid], current[mid:]
        first = matmul(upper, jnp.concatenate([upper, lower] * 2, axis=0), NT, HIGHEST)
        last = matmul(lower, jnp.concatenate([lower] * 4, axis=0), NT, HIGHEST)
        square = jnp.where((column < mid) & (row < column), last, first)
        gram[t, : fold, :] = jnp.where(lane[:fold] < vecs, square[:fold], square[fold:])
        gram[t, fold : fold + 1, :] = jnp.sum(
            jnp.where(row == column, last, 0.0), axis=0, keepdims=True
        )
        for d in range(plane - 1):
            stage1_copy(t, d).start()
        stage1[t, spot] = gram[t]

    def sum_planes(t):
        with jax.named_scope(f"s1_wait{t}"):
            for d in range(plane - 1):
                stage1_copy(t, d, True).wait_recv()
        total = stage1[t, 0]
        for p in range(1, plane):
            total = total + stage1[t, p]
        half[t] = total
        for d in range(planes - 1):
            stage2_copy(t, d).start()
        stage2[t, level] = total

    def sum_end(t):
        with jax.named_scope(f"s2_wait{t}"):
            for d in range(planes - 1):
                stage2_copy(t, d, True).wait_recv()
        total = stage2[t, 0]
        for p in range(1, planes):
            total = total + stage2[t, p]
        folded, diagonal = total[:fold], total[fold : fold + 1]
        square = jnp.concatenate([folded, pltpu.roll(folded, vecs, 1)], axis=0)
        filled = jnp.concatenate(
            [square, jnp.zeros((2 * vecs - mid, 2 * vecs), jnp.float32)], axis=0
        )
        turned = filled.T
        top = jnp.where((lane < mid) & (row < lane), turned[:mid], square)
        corner = jnp.where(row < lane, square, jnp.where(row == lane, diagonal, turned[:mid]))
        bottom = jnp.where(lane < mid, turned[mid:vecs], pltpu.roll(corner, mid, 1))
        return jnp.concatenate([top, bottom], axis=0)

    def inverse_factor(matrix):
        solved = factor_inverse(jnp.where(lane_all < vecs, matrix, identity))
        return pltpu.roll(solved, vecs, 1)[:, :vecs]

    def normalized(inverse, matrix):
        left = matmul(inverse, matrix[:, :vecs], NN, HIGHEST)
        padded = jnp.concatenate([inverse, jnp.zeros_like(inverse)], axis=0)
        return matmul(left, padded, NT, HIGHEST)

    sum_start(0, images)
    send_halo(1, images)
    own = own_part(images)
    sum_planes(0)
    ahead = next_images(1, images, own)
    sum_start(1, ahead)
    send_halo(2, ahead)
    own = own_part(ahead)
    matrix = sum_end(0)
    sum_planes(1)
    with jax.named_scope("chol0"):
        inverse = inverse_factor(matrix)
    with jax.named_scope("images2"):
        images = matmul(inverse, next_images(2, ahead, own), NN, HIGHEST)
        sum_start(2, images)
    matrix = sum_end(1)
    sum_planes(2)
    with jax.named_scope("chol1"):
        inverse = inverse_factor(normalized(inverse, matrix))
    images = matmul(inverse, images, NN, HIGHEST)
    matrix = sum_end(2)
    with jax.named_scope("chol2"):
        inverse = inverse_factor(normalized(inverse, matrix))
    out_ref[...] = matmul(inverse, images, NN, HIGHEST)

    with jax.named_scope("tail"):
        singles = [first_on, rest_on, last_on, back_copy, near_copy, next_copy, list_copy]
        for copy in singles + share_copies + part_copies:
            copy.wait_send()
        for t in range(ITERS):
            for copy in halo(t):
                copy.wait_send()
            for d in range(plane - 1):
                stage1_copy(t, d).wait_send()
            for d in range(planes - 1):
                stage2_copy(t, d).wait_send()


def solution(mesh):
    count, groups = mesh.shape["vox"], mesh.shape["subj"]
    plane = 8 if count >= 16 else count // 2
    planes = count // plane

    def on_device(series, live_mask, neighbours, start_vectors):
        subjects, voxels, frames = series.shape
        vecs = start_vectors.shape[1]
        offsets = neighbours.shape[1]
        scale_factor = 0.5 / math.sqrt(frames * subjects * groups)
        f32, bf16, i32 = jnp.float32, jnp.bfloat16, jnp.int32
        block = (vecs, voxels)
        table = (offsets, voxels)
        line = (1, voxels)
        packed = (vecs // 4 + 1, 2 * vecs)
        halves, width = 2 * subjects, frames // 2
        passed = halves * 5 // 8
        dma = pltpu.SemaphoreType.DMA
        outside = pl.BlockSpec(memory_space=pltpu.HBM)
        result = pl.pallas_call(
            functools.partial(kernel, (groups, plane, planes, scale_factor)),
            out_shape=jax.ShapeDtypeStruct(block, f32),
            in_specs=[outside] * 4,
            out_specs=pl.BlockSpec(memory_space=pltpu.VMEM),
            scratch_shapes=[
                pltpu.VMEM((subjects, voxels, frames), bf16),
                pltpu.VMEM((halves, voxels, width), bf16),
                pltpu.VMEM((passed, voxels, width), bf16),
                pltpu.VMEM((halves - passed, voxels, width), bf16),
                pltpu.VMEM(table, i32),
                pltpu.VMEM(table, i32),
                pltpu.VMEM(line, i32),
                pltpu.VMEM(block, f32),
                pltpu.VMEM((2 * voxels, voxels), f32),
                pltpu.VMEM((voxels, voxels), f32),
                pltpu.VMEM(table, f32),
                pltpu.VMEM(table, f32),
                pltpu.VMEM(table, f32),
                pltpu.VMEM((groups, *table), f32),
                pltpu.VMEM(table, f32),
                pltpu.VMEM(table, f32),
                pltpu.VMEM((2 * voxels, voxels), bf16),
                pltpu.VMEM((2 * voxels, voxels), bf16),
                pltpu.VMEM((voxels, voxels), bf16),
                pltpu.VMEM((voxels, voxels), bf16),
                pltpu.VMEM(line, f32),
                pltpu.VMEM((2, voxels), f32),
                pltpu.VMEM((2, voxels), f32),
                pltpu.VMEM((2, voxels), f32),
                pltpu.VMEM((2, voxels), f32),
                pltpu.VMEM((ITERS, *block), f32),
                pltpu.VMEM((ITERS, *block), f32),
                pltpu.VMEM((ITERS, *block), f32),
                pltpu.VMEM((ITERS, *packed), f32),
                pltpu.VMEM((ITERS, plane, *packed), f32),
                pltpu.VMEM((ITERS, *packed), f32),
                pltpu.VMEM((ITERS, planes, *packed), f32),
                dma((subjects + 3,)),
                dma((10,)),
                dma((10,)),
                dma((max(groups - 1, 1),)),
                dma((groups,)),
                dma((ITERS, 2)),
                dma((ITERS, 2)),
                dma((ITERS, plane - 1)),
                dma((ITERS, plane)),
                dma((ITERS, planes - 1)),
                dma((ITERS, planes)),
            ],
            compiler_params=pltpu.CompilerParams(
                collective_id=0, has_side_effects=True, vmem_limit_bytes=32 << 20
            ),
        )(
            *(
                pltpu.with_memory_space_constraint(operand, pltpu.HBM)
                for operand in (
                    series, live_mask.reshape(1, voxels), neighbours.T, start_vectors.T
                )
            )
        )
        return result.T

    placed = (P("subj", "vox", None), P("vox"), P("vox", None), P("vox", None))
    return jax.shard_map(
        on_device, mesh=mesh, in_specs=placed, out_specs=P("vox", None), check_vma=False
    )
```

```python
import functools
import math

import jax
import jax.numpy as jnp
from jax import lax
from jax.experimental import pallas as pl
from jax.experimental.pallas import tpu as pltpu
from jax.sharding import PartitionSpec as P

ITERS = 3
HIGHEST = lax.Precision.HIGHEST
NN = (((1,), (0,)), ((), ()))
NT = (((1,), (1,)), ((), ()))


def matmul(left, right, dims, precision=None):
    return lax.dot_general(
        left, right, dims, precision=precision, preferred_element_type=jnp.float32
    )


def split(values):
    high = values.astype(jnp.bfloat16)
    low = (values - high.astype(jnp.float32)).astype(jnp.bfloat16)
    return high, low


def factor_inverse(rows):
    total, width = rows.shape
    sublane = lax.broadcasted_iota(jnp.int32, (8, width), 0)

    def spread(first, left):
        return [
            jnp.broadcast_to(rows[:, first + c : first + c + 1], (left, width))
            for c in range(8)
        ]

    done = []
    cols = spread(0, total)
    for first in range(0, total, 8):
        left = total - first
        more = first + 8 < total
        if more:
            cols = cols + spread(first + 8, left)
        block = jnp.zeros((8, width), jnp.float32)
        for c in range(8):
            root = lax.rsqrt(cols[c][c : c + 1, :])
            lower = cols[c] * root
            pivot = rows[c : c + 1, :] * root
            block = jnp.where(sublane == c, pivot, block)
            rows = rows - lower * pivot
            for other in range(c + 1, len(cols)):
                cols[other] = cols[other] - lower * lower[other : other + 1, :]
        done.append(block)
        rows = rows[8:]
        cols = [column[8:] for column in cols[8:]]
    return jnp.concatenate(done, axis=0)


def kernel(
    sizes,
    series_ref,
    mask_ref,
    near_ref,
    start_ref,
    out_ref,
    raw,
    zown,
    zahead,
    zback,
    near,
    near_next,
    live,
    begin,
    corr,
    corr_next,
    part_next,
    part_in,
    part,
    parts,
    listed,
    listed_next,
    code,
    code_next,
    ghigh,
    glow,
    nhigh,
    nlow,
    scale_row,
    shares,
    shares_prev,
    shares_next,
    shares_second,
    halo_out,
    from_prev,
    from_next,
    gram,
    stage1,
    half,
    stage2,
    in_sems,
    send,
    recv,
    part_send,
    part_recv,
    halo_send,
    halo_recv,
    s1_send,
    s1_recv,
    s2_send,
    s2_recv,
):
    groups, plane, planes, scale_factor = sizes
    count = plane * planes
    subjects, voxels, frames = series_ref.shape
    offsets = near_ref.shape[0]
    vecs = start_ref.shape[0]
    halves, width = 2 * subjects, frames // 2
    passed = zahead.shape[0]
    me = lax.axis_index("vox")
    group = lax.axis_index("subj")
    core = lax.rem(me, 2)
    spot = lax.rem(me, plane)
    level = me // plane
    following = {"vox": lax.rem(me + 1, count)}
    previous = {"vox": lax.rem(me + count - 1, count)}
    second = {"vox": lax.rem(me + count - 2, count)}

    plane_peers = [lax.rem(spot + d, plane) for d in range(1, plane)]
    level_peers = [lax.rem(level + d, planes) for d in range(1, planes)]
    group_peers = [lax.rem(group + d, groups) for d in range(1, groups)]

    barrier = pltpu.get_barrier_semaphore()
    def far_first(peers):
        return sorted(peers, key=lambda d: -min(d, len(peers) + 1 - d))

    targets = []
    for d in far_first(range(1, max(groups, planes))):
        if d < groups:
            targets.append({"subj": group_peers[d - 1]})
        if d < planes:
            targets.append({"vox": level_peers[d - 1] * plane + spot})
    targets += [following, previous, {"vox": lax.rem(me + 2, count)}, second]
    targets += [{"vox": level * plane + p} for p in plane_peers]
    for target in targets:
        pl.semaphore_signal(
            barrier, inc=1, device_id=target, device_id_type=pl.DeviceIdType.MESH
        )

    loads = [
        pltpu.make_async_copy(series_ref.at[s], raw.at[s], in_sems.at[s])
        for s in range(subjects)
    ]
    small = [
        pltpu.make_async_copy(near_ref, near, in_sems.at[subjects]),
        pltpu.make_async_copy(mask_ref, live, in_sems.at[subjects + 1]),
        pltpu.make_async_copy(start_ref, begin, in_sems.at[subjects + 2]),
    ]
    for load in loads + small:
        load.start()

    def remote(src, dst, send_sem, recv_sem, target):
        return pltpu.make_async_remote_copy(
            src_ref=src,
            dst_ref=dst,
            send_sem=send_sem,
            recv_sem=recv_sem,
            device_id=target,
            device_id_type=pl.DeviceIdType.MESH,
        )

    def single(index, src, dst, target):
        return remote(src, dst, send.at[index], recv.at[index], target)

    def standardize(s):
        step = 64
        for r in range(0, voxels, step):
            values = raw[s, r : r + step, :].astype(jnp.float32)
            center = values - jnp.mean(values, axis=-1, keepdims=True)
            spread = jnp.mean(center * center, axis=-1, keepdims=True)
            result = (center * lax.rsqrt(spread + 1e-05)).astype(jnp.bfloat16)
            zown[2 * s, r : r + step, :] = result[:, :width]
            zown[2 * s + 1, r : r + step, :] = result[:, width:]

    with jax.named_scope("zscore"):
        for s in range(subjects):
            loads[s].wait()
            standardize(s)
        for load in small:
            load.wait()
    with jax.named_scope("barrier"):
        pl.semaphore_wait(barrier, len(targets))
    back_copy = single(2, zown.at[passed:halves], zback, previous)
    first_on = single(0, zown.at[0:2], zahead.at[0:2], following)
    rest_on = single(1, zown.at[2 : passed - 1], zahead.at[2 : passed - 1], following)
    last_on = single(9, zown.at[passed - 1 : passed], zahead.at[passed - 1 : passed], following)
    near_copy = single(3, near, near_next, previous)
    ons = [first_on, rest_on, last_on]
    backs = [near_copy, back_copy]

    def start_for(parity, copies):
        @pl.when(core == parity)
        def _():
            for copy in copies:
                copy.start()

    start_for(1, ons)
    start_for(0, backs)

    def products(left, right, first, last, left_first=0, right_first=0):
        total = None
        for h in range(first, last):
            term = matmul(left[left_first + h], right[right_first + h], NT)
            total = term if total is None else total + term
        return total

    tile = lax.broadcasted_iota(jnp.int32, (8, voxels), 0)

    def slots_of(ref):
        return [jnp.broadcast_to(ref[k : k + 1, :], (8, voxels)) for k in range(offsets)]

    def picked(source, slots, first, last, sums):
        def body(r, sums):
            ids = tile + r * 8
            values = source[pl.ds(pl.multiple_of(r * 8, 8), 8), :]
            return tuple(
                total + jnp.where(ids == slots[k], values, 0.0)
                for k, total in enumerate(sums)
            )

        return lax.fori_loop(first // 8, last // 8, body, sums, unroll=2)

    def down(sums, target):
        for k in range(offsets):
            target[k : k + 1, :] = jnp.sum(sums[k], axis=0, keepdims=True)

    def number_edges(slots, codes, rows_total):
        @pl.loop(0, rows_total // 8)
        def _(r):
            ids = tile + r * 8
            number = jnp.full((8, voxels), 15, jnp.int32)
            for k in range(offsets):
                number = jnp.where(ids == slots[k], k, number)
            codes[pl.ds(pl.multiple_of(r * 8, 8), 8), :] = number

    nothing = tuple(jnp.zeros((8, voxels), jnp.float32) for _ in range(offsets))
    with jax.named_scope("pick_own"):
        corr[voxels:, :] = products(zown, zown, 0, halves)
        sums = picked(corr, slots_of(near), voxels, 2 * voxels, nothing)
        down(sums, part)
        vectors = live[...].astype(jnp.float32) * begin[...]
        halo_out[0] = vectors
    start_for(0, ons)
    start_for(1, backs)
    number_edges(slots_of(near), code, 2 * voxels)
    with jax.named_scope("wait_first"):
        first_on.wait_recv()
    corr[:voxels, :] = products(zahead, zown, 0, 2)
    with jax.named_scope("wait_back"):
        near_copy.wait_recv()
        back_copy.wait_recv()
    with jax.named_scope("pick_next"):
        corr_next[...] = products(zown, zback, 0, halves - passed, left_first=passed)
        down(picked(corr_next, slots_of(near_next), 0, voxels, nothing), part_next)
    next_copy = single(4, part_next, part_in, following)
    next_copy.start()
    number_edges(slots_of(near_next), code_next, voxels)
    with jax.named_scope("wait_rest"):
        rest_on.wait_recv()
    corr[:voxels, :] += products(zahead, zown, 2, passed - 1)
    with jax.named_scope("wait_last"):
        last_on.wait_recv()
    with jax.named_scope("pick_cross"):
        corr[:voxels, :] += products(zahead, zown, passed - 1, passed)
        down(picked(corr, slots_of(near), 0, voxels, sums), part)
    with jax.named_scope("wait_part"):
        next_copy.wait_recv()
    part[...] += part_in[...]

    part_copies = []
    for d, peer in enumerate(group_peers):
        copy = remote(
            part, parts.at[group], part_send.at[d], part_recv.at[group], {"subj": peer}
        )
        copy.start()
        part_copies.append(copy)

    def halo(t):
        return (
            remote(halo_out.at[t], from_prev.at[t], halo_send.at[t, 0], halo_recv.at[t, 0], following),
            remote(halo_out.at[t], from_next.at[t], halo_send.at[t, 1], halo_recv.at[t, 1], previous),
        )

    for copy in halo(0):
        copy.start()
    parts[group] = part[...]
    with jax.named_scope("subj_wait"):
        for d, peer in enumerate(group_peers):
            remote(
                part, parts.at[peer], part_send.at[d], part_recv.at[peer], {"subj": peer}
            ).wait_recv()
    summed = parts[0]
    for g in range(1, groups):
        summed = summed + parts[g]
    weight = jnp.where(near[...] >= 0, jnp.exp(scale_factor * summed), 0.0)
    listed[...] = weight
    list_copy = single(5, listed, listed_next, previous)
    list_copy.start()

    def dense(codes, weight_table, high_out, low_out, rows_total):
        first = weight_table[:8, :]
        second_rows = jnp.concatenate(
            [weight_table[8:offsets, :], jnp.zeros((16 - offsets, voxels), jnp.float32)], axis=0
        )

        def gathered(source, index):
            return jnp.concatenate(
                [
                    jnp.take_along_axis(
                        source[:, c : c + 128], index[:, c : c + 128], axis=0,
                        mode="promise_in_bounds",
                    )
                    for c in range(0, voxels, 128)
                ],
                axis=1,
            )

        @pl.loop(0, rows_total // 16, unroll=2)
        def _(r):
            tiles = []
            for h in range(2):
                number = codes[pl.ds(pl.multiple_of(r * 16 + h * 8, 8), 8), :]
                inner = number & 7
                tiles.append(
                    jnp.where(number < 8, gathered(first, inner), gathered(second_rows, inner))
                )
            high, low = split(jnp.concatenate(tiles, axis=0))
            rows = pl.ds(pl.multiple_of(r * 16, 16), 16)
            high_out[rows, :] = high
            low_out[rows, :] = low

    ones = jnp.ones((8, voxels), jnp.bfloat16)
    with jax.named_scope("dense"):
        dense(code, listed, ghigh, glow, 2 * voxels)
        owed = matmul(ones, ghigh[...], NT) + matmul(ones, glow[...], NT)
        shares[:1, :] = (
            1.0 + jnp.sum(listed[...], axis=0, keepdims=True) + owed[:1, voxels:]
        )
        shares[1:2, :] = owed[:1, :voxels]
    share_copies = [
        single(6, shares, shares_prev, following),
        single(7, shares, shares_next, previous),
        single(8, shares, shares_second, second),
    ]
    for copy in share_copies:
        copy.start()
    with jax.named_scope("wait_list"):
        list_copy.wait_recv()
    with jax.named_scope("dense_next"):
        dense(code_next, listed_next, nhigh, nlow, voxels)

    def stacked(values):
        high, low = split(values)
        return high, jnp.concatenate([high, low], axis=0)

    def own_part(current):
        scaled = scale_row[...] * current
        high, both = stacked(scaled)
        mine = matmul(both, ghigh[voxels:, :], NT) + matmul(both, ghigh[voxels:, :], NN)
        rest = matmul(high, glow[voxels:, :], NT) + matmul(high, glow[voxels:, :], NN)
        return scaled + (mine[:vecs] + mine[vecs:] + rest)

    def whole_part(current, own, before, after):
        high, both = stacked(before)
        mine = matmul(both, ghigh[:voxels, :], NN)
        rest = matmul(high, glow[:voxels, :], NN)
        high, both = stacked(after)
        mine = mine + matmul(both, nhigh[...], NT)
        rest = rest + matmul(high, nlow[...], NT)
        total = own + (mine[:vecs] + mine[vecs:] + rest)
        return 0.5 * (current + scale_row[...] * total)

    with jax.named_scope("wait_shares"):
        for copy in share_copies + list(halo(0)):
            copy.wait_recv()
    with jax.named_scope("images0"):
        scale_row[...] = live[...].astype(jnp.float32) * lax.rsqrt(
            shares[:1, :] + shares_next[1:2, :]
        )
        scale_prev = lax.rsqrt(shares_prev[:1, :] + shares[1:2, :])
        scale_next = lax.rsqrt(shares_next[:1, :] + shares_second[1:2, :])
        images = whole_part(
            vectors, own_part(vectors), scale_prev * from_prev[0], scale_next * from_next[0]
        )

    mid = vecs // 2
    lane = lax.broadcasted_iota(jnp.int32, (mid, 2 * vecs), 1)
    row = lax.broadcasted_iota(jnp.int32, (mid, 2 * vecs), 0)
    column = lax.rem(lane, vecs)
    row_all = lax.broadcasted_iota(jnp.int32, (vecs, 2 * vecs), 0)
    lane_all = lax.broadcasted_iota(jnp.int32, (vecs, 2 * vecs), 1)
    identity = (lane_all - vecs == row_all).astype(jnp.float32)
    fold = mid // 2

    def send_halo(t, current):
        halo_out[t] = scale_row[...] * current
        for copy in halo(t):
            copy.start()

    def next_images(t, current, own):
        with jax.named_scope("wait_halo"):
            for copy in halo(t):
                copy.wait_recv()
        return whole_part(current, own, from_prev[t], from_next[t])

    def stage1_copy(t, d, arriving=False):
        peer = plane_peers[d]
        target = {"vox": level * plane + peer}
        slot = peer if arriving else spot
        return remote(gram.at[t], stage1.at[t, slot], s1_send.at[t, d], s1_recv.at[t, slot], target)

    def stage2_copy(t, d, arriving=False):
        peer = level_peers[d]
        target = {"vox": peer * plane + spot}
        slot = peer if arriving else level
        return remote(half.at[t], stage2.at[t, slot], s2_send.at[t, d], s2_recv.at[t, slot], target)

    def sum_start(t, current):
        upper, lower = current[:mid], current[mid:]
        first = matmul(upper, jnp.concatenate([upper, lower] * 2, axis=0), NT, HIGHEST)
        last = matmul(lower, jnp.concatenate([lower] * 4, axis=0), NT, HIGHEST)
        square = jnp.where((column < mid) & (row < column), last, first)
        gram[t, : fold, :] = jnp.where(lane[:fold] < vecs, square[:fold], square[fold:])
        gram[t, fold : fold + 1, :] = jnp.sum(
            jnp.where(row == column, last, 0.0), axis=0, keepdims=True
        )
        for d in range(plane - 1):
            stage1_copy(t, d).start()
        stage1[t, spot] = gram[t]

    def sum_planes(t):
        with jax.named_scope(f"s1_wait{t}"):
            for d in range(plane - 1):
                stage1_copy(t, d, True).wait_recv()
        total = stage1[t, 0]
        for p in range(1, plane):
            total = total + stage1[t, p]
        half[t] = total
        for d in range(planes - 1):
            stage2_copy(t, d).start()
        stage2[t, level] = total

    def sum_end(t):
        with jax.named_scope(f"s2_wait{t}"):
            for d in range(planes - 1):
                stage2_copy(t, d, True).wait_recv()
        total = stage2[t, 0]
        for p in range(1, planes):
            total = total + stage2[t, p]
        folded, diagonal = total[:fold], total[fold : fold + 1]
        square = jnp.concatenate([folded, pltpu.roll(folded, vecs, 1)], axis=0)
        filled = jnp.concatenate(
            [square, jnp.zeros((2 * vecs - mid, 2 * vecs), jnp.float32)], axis=0
        )
        turned = filled.T
        top = jnp.where((lane < mid) & (row < lane), turned[:mid], square)
        corner = jnp.where(row < lane, square, jnp.where(row == lane, diagonal, turned[:mid]))
        bottom = jnp.where(lane < mid, turned[mid:vecs], pltpu.roll(corner, mid, 1))
        return jnp.concatenate([top, bottom], axis=0)

    def inverse_factor(matrix):
        solved = factor_inverse(jnp.where(lane_all < vecs, matrix, identity))
        return pltpu.roll(solved, vecs, 1)[:, :vecs]

    def normalized(inverse, matrix):
        left = matmul(inverse, matrix[:, :vecs], NN, HIGHEST)
        padded = jnp.concatenate([inverse, jnp.zeros_like(inverse)], axis=0)
        return matmul(left, padded, NT, HIGHEST)

    sum_start(0, images)
    send_halo(1, images)
    own = own_part(images)
    sum_planes(0)
    ahead = next_images(1, images, own)
    sum_start(1, ahead)
    send_halo(2, ahead)
    own = own_part(ahead)
    matrix = sum_end(0)
    sum_planes(1)
    with jax.named_scope("chol0"):
        inverse = inverse_factor(matrix)
    with jax.named_scope("images2"):
        images = matmul(inverse, next_images(2, ahead, own), NN, HIGHEST)
        sum_start(2, images)
    matrix = sum_end(1)
    sum_planes(2)
    with jax.named_scope("chol1"):
        inverse = inverse_factor(normalized(inverse, matrix))
    images = matmul(inverse, images, NN, HIGHEST)
    matrix = sum_end(2)
    with jax.named_scope("chol2"):
        inverse = inverse_factor(normalized(inverse, matrix))
    out_ref[...] = matmul(inverse, images, NN, HIGHEST)

    with jax.named_scope("tail"):
        singles = [first_on, rest_on, last_on, back_copy, near_copy, next_copy, list_copy]
        for copy in singles + share_copies + part_copies:
            copy.wait_send()
        for t in range(ITERS):
            for copy in halo(t):
                copy.wait_send()
            for d in range(plane - 1):
                stage1_copy(t, d).wait_send()
            for d in range(planes - 1):
                stage2_copy(t, d).wait_send()


def solution(mesh):
    count, groups = mesh.shape["vox"], mesh.shape["subj"]
    plane = 8 if count >= 16 else count // 2
    planes = count // plane

    def on_device(series, live_mask, neighbours, start_vectors):
        subjects, voxels, frames = series.shape
        vecs = start_vectors.shape[1]
        offsets = neighbours.shape[1]
        scale_factor = 0.5 / math.sqrt(frames * subjects * groups)
        f32, bf16, i32 = jnp.float32, jnp.bfloat16, jnp.int32
        block = (vecs, voxels)
        table = (offsets, voxels)
        line = (1, voxels)
        packed = (vecs // 4 + 1, 2 * vecs)
        halves, width = 2 * subjects, frames // 2
        passed = halves * 5 // 8
        dma = pltpu.SemaphoreType.DMA
        outside = pl.BlockSpec(memory_space=pltpu.HBM)
        result = pl.pallas_call(
            functools.partial(kernel, (groups, plane, planes, scale_factor)),
            out_shape=jax.ShapeDtypeStruct(block, f32),
            in_specs=[outside] * 4,
            out_specs=pl.BlockSpec(memory_space=pltpu.VMEM),
            scratch_shapes=[
                pltpu.VMEM((subjects, voxels, frames), bf16),
                pltpu.VMEM((halves, voxels, width), bf16),
                pltpu.VMEM((passed, voxels, width), bf16),
                pltpu.VMEM((halves - passed, voxels, width), bf16),
                pltpu.VMEM(table, i32),
                pltpu.VMEM(table, i32),
                pltpu.VMEM(line, i32),
                pltpu.VMEM(block, f32),
                pltpu.VMEM((2 * voxels, voxels), f32),
                pltpu.VMEM((voxels, voxels), f32),
                pltpu.VMEM(table, f32),
                pltpu.VMEM(table, f32),
                pltpu.VMEM(table, f32),
                pltpu.VMEM((groups, *table), f32),
                pltpu.VMEM(table, f32),
                pltpu.VMEM(table, f32),
                pltpu.VMEM((2 * voxels, voxels), i32),
                pltpu.VMEM((voxels, voxels), i32),
                pltpu.VMEM((2 * voxels, voxels), bf16),
                pltpu.VMEM((2 * voxels, voxels), bf16),
                pltpu.VMEM((voxels, voxels), bf16),
                pltpu.VMEM((voxels, voxels), bf16),
                pltpu.VMEM(line, f32),
                pltpu.VMEM((2, voxels), f32),
                pltpu.VMEM((2, voxels), f32),
                pltpu.VMEM((2, voxels), f32),
                pltpu.VMEM((2, voxels), f32),
                pltpu.VMEM((ITERS, *block), f32),
                pltpu.VMEM((ITERS, *block), f32),
                pltpu.VMEM((ITERS, *block), f32),
                pltpu.VMEM((ITERS, *packed), f32),
                pltpu.VMEM((ITERS, plane, *packed), f32),
                pltpu.VMEM((ITERS, *packed), f32),
                pltpu.VMEM((ITERS, planes, *packed), f32),
                dma((subjects + 3,)),
                dma((10,)),
                dma((10,)),
                dma((max(groups - 1, 1),)),
                dma((groups,)),
                dma((ITERS, 2)),
                dma((ITERS, 2)),
                dma((ITERS, plane - 1)),
                dma((ITERS, plane)),
                dma((ITERS, planes - 1)),
                dma((ITERS, planes)),
            ],
            compiler_params=pltpu.CompilerParams(
                collective_id=0, has_side_effects=True, vmem_limit_bytes=32 << 20
            ),
        )(
            *(
                pltpu.with_memory_space_constraint(operand, pltpu.HBM)
                for operand in (
                    series, live_mask.reshape(1, voxels), neighbours.T, start_vectors.T
                )
            )
        )
        return result.T

    placed = (P("subj", "vox", None), P("vox"), P("vox", None), P("vox", None))
    return jax.shard_map(
        on_device, mesh=mesh, in_specs=placed, out_specs=P("vox", None), check_vma=False
    )
```

```python
import functools
import math

import jax
import jax.numpy as jnp
from jax import lax
from jax.experimental import pallas as pl
from jax.experimental.pallas import tpu as pltpu
from jax.sharding import PartitionSpec as P

ITERS = 3
HIGHEST = lax.Precision.HIGHEST
NN = (((1,), (0,)), ((), ()))
NT = (((1,), (1,)), ((), ()))


def matmul(left, right, dims, precision=None):
    return lax.dot_general(
        left, right, dims, precision=precision, preferred_element_type=jnp.float32
    )


def split(values):
    high = values.astype(jnp.bfloat16)
    low = (values - high.astype(jnp.float32)).astype(jnp.bfloat16)
    return high, low


def factor_inverse(rows):
    total, width = rows.shape
    sublane = lax.broadcasted_iota(jnp.int32, (8, width), 0)

    def spread(first, left):
        return [
            jnp.broadcast_to(rows[:, first + c : first + c + 1], (left, width))
            for c in range(8)
        ]

    done = []
    cols = spread(0, total)
    for first in range(0, total, 8):
        left = total - first
        more = first + 8 < total
        if more:
            cols = cols + spread(first + 8, left)
        block = jnp.zeros((8, width), jnp.float32)
        for c in range(8):
            root = lax.rsqrt(cols[c][c : c + 1, :])
            lower = cols[c] * root
            pivot = rows[c : c + 1, :] * root
            block = jnp.where(sublane == c, pivot, block)
            rows = rows - lower * pivot
            for other in range(c + 1, len(cols)):
                cols[other] = cols[other] - lower * lower[other : other + 1, :]
        done.append(block)
        rows = rows[8:]
        cols = [column[8:] for column in cols[8:]]
    return jnp.concatenate(done, axis=0)


def kernel(
    sizes,
    series_ref,
    mask_ref,
    near_ref,
    start_ref,
    out_ref,
    raw,
    zown,
    zahead,
    zback,
    near,
    near_next,
    live,
    begin,
    corr,
    corr_next,
    part_next,
    part_in,
    part,
    parts,
    listed,
    listed_next,
    code,
    code_next,
    ghigh,
    glow,
    nhigh,
    nlow,
    scale_row,
    shares,
    shares_prev,
    shares_next,
    shares_second,
    halo_out,
    from_prev,
    from_next,
    gram,
    stage1,
    half,
    stage2,
    in_sems,
    send,
    recv,
    part_send,
    part_recv,
    halo_send,
    halo_recv,
    s1_send,
    s1_recv,
    s2_send,
    s2_recv,
):
    groups, plane, planes, scale_factor = sizes
    count = plane * planes
    subjects, voxels, frames = series_ref.shape
    offsets = near_ref.shape[0]
    vecs = start_ref.shape[0]
    halves, width = 2 * subjects, frames // 2
    passed = zahead.shape[0]
    me = lax.axis_index("vox")
    group = lax.axis_index("subj")
    core = lax.rem(me, 2)
    spot = lax.rem(me, plane)
    level = me // plane
    following = {"vox": lax.rem(me + 1, count)}
    previous = {"vox": lax.rem(me + count - 1, count)}
    second = {"vox": lax.rem(me + count - 2, count)}

    plane_peers = [lax.rem(spot + d, plane) for d in range(1, plane)]
    level_peers = [lax.rem(level + d, planes) for d in range(1, planes)]
    group_peers = [lax.rem(group + d, groups) for d in range(1, groups)]

    barrier = pltpu.get_barrier_semaphore()
    def far_first(peers):
        return sorted(range(len(peers)), key=lambda d: -min(d + 1, len(peers) - d))

    targets = []
    for d in far_first(range(max(groups, planes) - 1)):
        if d < groups - 1:
            targets.append({"subj": group_peers[d]})
        if d < planes - 1:
            targets.append({"vox": level_peers[d] * plane + spot})
    targets += [following, previous, {"vox": lax.rem(me + 2, count)}, second]
    targets += [{"vox": level * plane + p} for p in plane_peers]
    for target in targets:
        pl.semaphore_signal(
            barrier, inc=1, device_id=target, device_id_type=pl.DeviceIdType.MESH
        )

    loads = [
        pltpu.make_async_copy(series_ref.at[s], raw.at[s], in_sems.at[s])
        for s in range(subjects)
    ]
    small = [
        pltpu.make_async_copy(near_ref, near, in_sems.at[subjects]),
        pltpu.make_async_copy(mask_ref, live, in_sems.at[subjects + 1]),
        pltpu.make_async_copy(start_ref, begin, in_sems.at[subjects + 2]),
    ]
    for load in loads + small:
        load.start()

    def remote(src, dst, send_sem, recv_sem, target):
        return pltpu.make_async_remote_copy(
            src_ref=src,
            dst_ref=dst,
            send_sem=send_sem,
            recv_sem=recv_sem,
            device_id=target,
            device_id_type=pl.DeviceIdType.MESH,
        )

    def single(index, src, dst, target):
        return remote(src, dst, send.at[index], recv.at[index], target)

    def standardize(s):
        step = 64
        for r in range(0, voxels, step):
            values = raw[s, r : r + step, :].astype(jnp.float32)
            center = values - jnp.mean(values, axis=-1, keepdims=True)
            spread = jnp.mean(center * center, axis=-1, keepdims=True)
            result = (center * lax.rsqrt(spread + 1e-05)).astype(jnp.bfloat16)
            zown[2 * s, r : r + step, :] = result[:, :width]
            zown[2 * s + 1, r : r + step, :] = result[:, width:]

    with jax.named_scope("zscore"):
        for s in range(subjects):
            loads[s].wait()
            standardize(s)
        for load in small:
            load.wait()
    with jax.named_scope("barrier"):
        pl.semaphore_wait(barrier, len(targets))
    split_at = halves - passed - 1
    back_copy = single(2, zown.at[passed : halves - 1], zback.at[0:split_at], previous)
    back_last = single(
        10, zown.at[halves - 1 : halves], zback.at[split_at : split_at + 1], previous
    )
    first_on = single(0, zown.at[0:2], zahead.at[0:2], following)
    rest_on = single(1, zown.at[2 : passed - 1], zahead.at[2 : passed - 1], following)
    last_on = single(9, zown.at[passed - 1 : passed], zahead.at[passed - 1 : passed], following)
    near_copy = single(3, near, near_next, previous)
    ons = [first_on, rest_on, last_on]
    backs = [near_copy, back_copy, back_last]

    def start_for(parity, copies):
        @pl.when(core == parity)
        def _():
            for copy in copies:
                copy.start()

    start_for(1, ons)
    start_for(0, backs)

    def products(left, right, first, last, left_first=0, right_first=0):
        total = None
        for h in range(first, last):
            term = matmul(left[left_first + h], right[right_first + h], NT)
            total = term if total is None else total + term
        return total

    tile = lax.broadcasted_iota(jnp.int32, (8, voxels), 0)

    def slots_of(ref):
        return [jnp.broadcast_to(ref[k : k + 1, :], (8, voxels)) for k in range(offsets)]

    def picked(source, slots, first, last, sums):
        def body(r, sums):
            ids = tile + r * 8
            values = source[pl.ds(pl.multiple_of(r * 8, 8), 8), :]
            return tuple(
                total + jnp.where(ids == slots[k], values, 0.0)
                for k, total in enumerate(sums)
            )

        return lax.fori_loop(first // 8, last // 8, body, sums, unroll=2)

    def down(sums, target):
        for k in range(offsets):
            target[k : k + 1, :] = jnp.sum(sums[k], axis=0, keepdims=True)

    def number_edges(slots, codes, rows_total):
        @pl.loop(0, rows_total // 8)
        def _(r):
            ids = tile + r * 8
            number = jnp.full((8, voxels), 15, jnp.int32)
            for k in range(offsets):
                number = jnp.where(ids == slots[k], k, number)
            codes[pl.ds(pl.multiple_of(r * 8, 8), 8), :] = number

    nothing = tuple(jnp.zeros((8, voxels), jnp.float32) for _ in range(offsets))
    with jax.named_scope("pick_own"):
        corr[voxels:, :] = products(zown, zown, 0, halves)
        sums = picked(corr, slots_of(near), voxels, 2 * voxels, nothing)
        down(sums, part)
        vectors = live[...].astype(jnp.float32) * begin[...]
        halo_out[0] = vectors
    start_for(0, ons)
    start_for(1, backs)
    number_edges(slots_of(near), code, 2 * voxels)
    with jax.named_scope("wait_first"):
        first_on.wait_recv()
    corr[:voxels, :] = products(zahead, zown, 0, 2)
    with jax.named_scope("wait_back"):
        near_copy.wait_recv()
        back_copy.wait_recv()
    corr_next[...] = products(zown, zback, 0, split_at, left_first=passed)
    with jax.named_scope("wait_back_last"):
        back_last.wait_recv()
    with jax.named_scope("pick_next"):
        corr_next[...] += products(zown, zback, split_at, split_at + 1, left_first=passed)
        down(picked(corr_next, slots_of(near_next), 0, voxels, nothing), part_next)
    next_copy = single(4, part_next, part_in, following)
    next_copy.start()
    number_edges(slots_of(near_next), code_next, voxels)
    with jax.named_scope("wait_rest"):
        rest_on.wait_recv()
    corr[:voxels, :] += products(zahead, zown, 2, passed - 1)
    with jax.named_scope("wait_last"):
        last_on.wait_recv()
    with jax.named_scope("pick_cross"):
        corr[:voxels, :] += products(zahead, zown, passed - 1, passed)
        down(picked(corr, slots_of(near), 0, voxels, sums), part)
    with jax.named_scope("wait_part"):
        next_copy.wait_recv()
    part[...] += part_in[...]

    part_copies = []
    for d in far_first(group_peers):
        copy = remote(
            part, parts.at[group], part_send.at[d], part_recv.at[group], {"subj": group_peers[d]}
        )
        copy.start()
        part_copies.append(copy)

    def halo(t):
        return (
            remote(halo_out.at[t], from_prev.at[t], halo_send.at[t, 0], halo_recv.at[t, 0], following),
            remote(halo_out.at[t], from_next.at[t], halo_send.at[t, 1], halo_recv.at[t, 1], previous),
        )

    for copy in halo(0):
        copy.start()
    parts[group] = part[...]
    with jax.named_scope("subj_wait"):
        for d, peer in enumerate(group_peers):
            remote(
                part, parts.at[peer], part_send.at[d], part_recv.at[peer], {"subj": peer}
            ).wait_recv()
    summed = parts[0]
    for g in range(1, groups):
        summed = summed + parts[g]
    weight = jnp.where(near[...] >= 0, jnp.exp(scale_factor * summed), 0.0)
    listed[...] = weight
    list_copy = single(5, listed, listed_next, previous)
    list_copy.start()

    def dense(codes, weight_table, high_out, low_out, rows_total):
        first = weight_table[:8, :]
        second_rows = jnp.concatenate(
            [weight_table[8:offsets, :], jnp.zeros((16 - offsets, voxels), jnp.float32)], axis=0
        )

        def gathered(source, index):
            return jnp.concatenate(
                [
                    jnp.take_along_axis(
                        source[:, c : c + 128], index[:, c : c + 128], axis=0,
                        mode="promise_in_bounds",
                    )
                    for c in range(0, voxels, 128)
                ],
                axis=1,
            )

        @pl.loop(0, rows_total // 16, unroll=2)
        def _(r):
            tiles = []
            for h in range(2):
                number = codes[pl.ds(pl.multiple_of(r * 16 + h * 8, 8), 8), :]
                inner = number & 7
                tiles.append(
                    jnp.where(number < 8, gathered(first, inner), gathered(second_rows, inner))
                )
            high, low = split(jnp.concatenate(tiles, axis=0))
            rows = pl.ds(pl.multiple_of(r * 16, 16), 16)
            high_out[rows, :] = high
            low_out[rows, :] = low

    ones = jnp.ones((8, voxels), jnp.bfloat16)
    with jax.named_scope("dense"):
        dense(code, listed, ghigh, glow, 2 * voxels)
        owed = matmul(ones, ghigh[...], NT) + matmul(ones, glow[...], NT)
        shares[:1, :] = (
            1.0 + jnp.sum(listed[...], axis=0, keepdims=True) + owed[:1, voxels:]
        )
        shares[1:2, :] = owed[:1, :voxels]
    share_copies = [
        single(6, shares, shares_prev, following),
        single(7, shares, shares_next, previous),
        single(8, shares, shares_second, second),
    ]
    for copy in share_copies:
        copy.start()
    with jax.named_scope("wait_list"):
        list_copy.wait_recv()
    with jax.named_scope("dense_next"):
        dense(code_next, listed_next, nhigh, nlow, voxels)

    def stacked(values):
        high, low = split(values)
        return high, jnp.concatenate([high, low], axis=0)

    def own_part(current):
        scaled = scale_row[...] * current
        high, both = stacked(scaled)
        mine = matmul(both, ghigh[voxels:, :], NT) + matmul(both, ghigh[voxels:, :], NN)
        rest = matmul(high, glow[voxels:, :], NT) + matmul(high, glow[voxels:, :], NN)
        return scaled + (mine[:vecs] + mine[vecs:] + rest)

    def whole_part(current, own, before, after):
        high, both = stacked(before)
        mine = matmul(both, ghigh[:voxels, :], NN)
        rest = matmul(high, glow[:voxels, :], NN)
        high, both = stacked(after)
        mine = mine + matmul(both, nhigh[...], NT)
        rest = rest + matmul(high, nlow[...], NT)
        total = own + (mine[:vecs] + mine[vecs:] + rest)
        return 0.5 * (current + scale_row[...] * total)

    with jax.named_scope("wait_shares"):
        for copy in share_copies + list(halo(0)):
            copy.wait_recv()
    with jax.named_scope("images0"):
        scale_row[...] = live[...].astype(jnp.float32) * lax.rsqrt(
            shares[:1, :] + shares_next[1:2, :]
        )
        scale_prev = lax.rsqrt(shares_prev[:1, :] + shares[1:2, :])
        scale_next = lax.rsqrt(shares_next[:1, :] + shares_second[1:2, :])
        images = whole_part(
            vectors, own_part(vectors), scale_prev * from_prev[0], scale_next * from_next[0]
        )

    mid = vecs // 2
    lane = lax.broadcasted_iota(jnp.int32, (mid, 2 * vecs), 1)
    row = lax.broadcasted_iota(jnp.int32, (mid, 2 * vecs), 0)
    column = lax.rem(lane, vecs)
    row_all = lax.broadcasted_iota(jnp.int32, (vecs, 2 * vecs), 0)
    lane_all = lax.broadcasted_iota(jnp.int32, (vecs, 2 * vecs), 1)
    identity = (lane_all - vecs == row_all).astype(jnp.float32)
    fold = mid // 2

    def send_halo(t, current):
        halo_out[t] = scale_row[...] * current
        for copy in halo(t):
            copy.start()

    def next_images(t, current, own):
        with jax.named_scope("wait_halo"):
            for copy in halo(t):
                copy.wait_recv()
        return whole_part(current, own, from_prev[t], from_next[t])

    def stage1_copy(t, d, arriving=False):
        peer = plane_peers[d]
        target = {"vox": level * plane + peer}
        slot = peer if arriving else spot
        return remote(gram.at[t], stage1.at[t, slot], s1_send.at[t, d], s1_recv.at[t, slot], target)

    def stage2_copy(t, d, arriving=False):
        peer = level_peers[d]
        target = {"vox": peer * plane + spot}
        slot = peer if arriving else level
        return remote(half.at[t], stage2.at[t, slot], s2_send.at[t, d], s2_recv.at[t, slot], target)

    def sum_start(t, current):
        upper, lower = current[:mid], current[mid:]
        first = matmul(upper, jnp.concatenate([upper, lower] * 2, axis=0), NT, HIGHEST)
        last = matmul(lower, jnp.concatenate([lower] * 4, axis=0), NT, HIGHEST)
        square = jnp.where((column < mid) & (row < column), last, first)
        gram[t, : fold, :] = jnp.where(lane[:fold] < vecs, square[:fold], square[fold:])
        gram[t, fold : fold + 1, :] = jnp.sum(
            jnp.where(row == column, last, 0.0), axis=0, keepdims=True
        )
        for d in far_first(plane_peers):
            stage1_copy(t, d).start()
        stage1[t, spot] = gram[t]

    def sum_planes(t):
        with jax.named_scope(f"s1_wait{t}"):
            for d in range(plane - 1):
                stage1_copy(t, d, True).wait_recv()
        total = stage1[t, 0]
        for p in range(1, plane):
            total = total + stage1[t, p]
        half[t] = total
        for d in far_first(level_peers):
            stage2_copy(t, d).start()
        stage2[t, level] = total

    def sum_end(t):
        with jax.named_scope(f"s2_wait{t}"):
            for d in range(planes - 1):
                stage2_copy(t, d, True).wait_recv()
        total = stage2[t, 0]
        for p in range(1, planes):
            total = total + stage2[t, p]
        folded, diagonal = total[:fold], total[fold : fold + 1]
        square = jnp.concatenate([folded, pltpu.roll(folded, vecs, 1)], axis=0)
        filled = jnp.concatenate(
            [square, jnp.zeros((2 * vecs - mid, 2 * vecs), jnp.float32)], axis=0
        )
        turned = filled.T
        top = jnp.where((lane < mid) & (row < lane), turned[:mid], square)
        corner = jnp.where(row < lane, square, jnp.where(row == lane, diagonal, turned[:mid]))
        bottom = jnp.where(lane < mid, turned[mid:vecs], pltpu.roll(corner, mid, 1))
        return jnp.concatenate([top, bottom], axis=0)

    def inverse_factor(matrix):
        solved = factor_inverse(jnp.where(lane_all < vecs, matrix, identity))
        return pltpu.roll(solved, vecs, 1)[:, :vecs]

    def normalized(inverse, matrix):
        left = matmul(inverse, matrix[:, :vecs], NN, HIGHEST)
        padded = jnp.concatenate([inverse, jnp.zeros_like(inverse)], axis=0)
        return matmul(left, padded, NT, HIGHEST)

    sum_start(0, images)
    send_halo(1, images)
    own = own_part(images)
    sum_planes(0)
    ahead = next_images(1, images, own)
    sum_start(1, ahead)
    send_halo(2, ahead)
    own = own_part(ahead)
    matrix = sum_end(0)
    sum_planes(1)
    with jax.named_scope("chol0"):
        inverse = inverse_factor(matrix)
    with jax.named_scope("images2"):
        images = matmul(inverse, next_images(2, ahead, own), NN, HIGHEST)
        sum_start(2, images)
    sum_planes(2)
    matrix = sum_end(1)
    with jax.named_scope("chol1"):
        inverse = inverse_factor(normalized(inverse, matrix))
    images = matmul(inverse, images, NN, HIGHEST)
    matrix = sum_end(2)
    with jax.named_scope("chol2"):
        inverse = inverse_factor(normalized(inverse, matrix))
    out_ref[...] = matmul(inverse, images, NN, HIGHEST)

    with jax.named_scope("tail"):
        singles = [first_on, rest_on, last_on, back_copy, back_last, near_copy, next_copy, list_copy]
        for copy in singles + share_copies + part_copies:
            copy.wait_send()
        for t in range(ITERS):
            for copy in halo(t):
                copy.wait_send()
            for d in range(plane - 1):
                stage1_copy(t, d).wait_send()
            for d in range(planes - 1):
                stage2_copy(t, d).wait_send()


def solution(mesh):
    count, groups = mesh.shape["vox"], mesh.shape["subj"]
    plane = 8 if count >= 16 else count // 2
    planes = count // plane

    def on_device(series, live_mask, neighbours, start_vectors):
        subjects, voxels, frames = series.shape
        vecs = start_vectors.shape[1]
        offsets = neighbours.shape[1]
        scale_factor = 0.5 / math.sqrt(frames * subjects * groups)
        f32, bf16, i32 = jnp.float32, jnp.bfloat16, jnp.int32
        block = (vecs, voxels)
        table = (offsets, voxels)
        line = (1, voxels)
        packed = (vecs // 4 + 1, 2 * vecs)
        halves, width = 2 * subjects, frames // 2
        passed = halves * 5 // 8
        dma = pltpu.SemaphoreType.DMA
        outside = pl.BlockSpec(memory_space=pltpu.HBM)
        result = pl.pallas_call(
            functools.partial(kernel, (groups, plane, planes, scale_factor)),
            out_shape=jax.ShapeDtypeStruct(block, f32),
            in_specs=[outside] * 4,
            out_specs=pl.BlockSpec(memory_space=pltpu.VMEM),
            scratch_shapes=[
                pltpu.VMEM((subjects, voxels, frames), bf16),
                pltpu.VMEM((halves, voxels, width), bf16),
                pltpu.VMEM((passed, voxels, width), bf16),
                pltpu.VMEM((halves - passed, voxels, width), bf16),
                pltpu.VMEM(table, i32),
                pltpu.VMEM(table, i32),
                pltpu.VMEM(line, i32),
                pltpu.VMEM(block, f32),
                pltpu.VMEM((2 * voxels, voxels), f32),
                pltpu.VMEM((voxels, voxels), f32),
                pltpu.VMEM(table, f32),
                pltpu.VMEM(table, f32),
                pltpu.VMEM(table, f32),
                pltpu.VMEM((groups, *table), f32),
                pltpu.VMEM(table, f32),
                pltpu.VMEM(table, f32),
                pltpu.VMEM((2 * voxels, voxels), i32),
                pltpu.VMEM((voxels, voxels), i32),
                pltpu.VMEM((2 * voxels, voxels), bf16),
                pltpu.VMEM((2 * voxels, voxels), bf16),
                pltpu.VMEM((voxels, voxels), bf16),
                pltpu.VMEM((voxels, voxels), bf16),
                pltpu.VMEM(line, f32),
                pltpu.VMEM((2, voxels), f32),
                pltpu.VMEM((2, voxels), f32),
                pltpu.VMEM((2, voxels), f32),
                pltpu.VMEM((2, voxels), f32),
                pltpu.VMEM((ITERS, *block), f32),
                pltpu.VMEM((ITERS, *block), f32),
                pltpu.VMEM((ITERS, *block), f32),
                pltpu.VMEM((ITERS, *packed), f32),
                pltpu.VMEM((ITERS, plane, *packed), f32),
                pltpu.VMEM((ITERS, *packed), f32),
                pltpu.VMEM((ITERS, planes, *packed), f32),
                dma((subjects + 3,)),
                dma((11,)),
                dma((11,)),
                dma((max(groups - 1, 1),)),
                dma((groups,)),
                dma((ITERS, 2)),
                dma((ITERS, 2)),
                dma((ITERS, plane - 1)),
                dma((ITERS, plane)),
                dma((ITERS, planes - 1)),
                dma((ITERS, planes)),
            ],
            compiler_params=pltpu.CompilerParams(
                collective_id=0, has_side_effects=True, vmem_limit_bytes=32 << 20
            ),
        )(
            *(
                pltpu.with_memory_space_constraint(operand, pltpu.HBM)
                for operand in (
                    series, live_mask.reshape(1, voxels), neighbours.T, start_vectors.T
                )
            )
        )
        return result.T

    placed = (P("subj", "vox", None), P("vox"), P("vox", None), P("vox", None))
    return jax.shard_map(
        on_device, mesh=mesh, in_specs=placed, out_specs=P("vox", None), check_vma=False
    )
```

```python
import functools
import math

import jax
import jax.numpy as jnp
from jax import lax
from jax.experimental import pallas as pl
from jax.experimental.pallas import tpu as pltpu
from jax.sharding import PartitionSpec as P

ITERS = 3
HIGHEST = lax.Precision.HIGHEST
NN = (((1,), (0,)), ((), ()))
NT = (((1,), (1,)), ((), ()))


def matmul(left, right, dims, precision=None):
    return lax.dot_general(
        left, right, dims, precision=precision, preferred_element_type=jnp.float32
    )


def split(values):
    high = values.astype(jnp.bfloat16)
    low = (values - high.astype(jnp.float32)).astype(jnp.bfloat16)
    return high, low


def factor_inverse(rows):
    total, width = rows.shape
    sublane = lax.broadcasted_iota(jnp.int32, (8, width), 0)

    def spread(first, left):
        return [
            jnp.broadcast_to(rows[:, first + c : first + c + 1], (left, width))
            for c in range(8)
        ]

    done = []
    cols = spread(0, total)
    for first in range(0, total, 8):
        left = total - first
        more = first + 8 < total
        if more:
            cols = cols + spread(first + 8, left)
        block = jnp.zeros((8, width), jnp.float32)
        for c in range(8):
            root = lax.rsqrt(cols[c][c : c + 1, :])
            lower = cols[c] * root
            pivot = rows[c : c + 1, :] * root
            block = jnp.where(sublane == c, pivot, block)
            rows = rows - lower * pivot
            for other in range(c + 1, len(cols)):
                cols[other] = cols[other] - lower * lower[other : other + 1, :]
        done.append(block)
        rows = rows[8:]
        cols = [column[8:] for column in cols[8:]]
    return jnp.concatenate(done, axis=0)


def kernel(
    sizes,
    series_ref,
    mask_ref,
    near_ref,
    start_ref,
    out_ref,
    raw,
    zown,
    zahead,
    zback,
    near,
    near_next,
    live,
    begin,
    corr,
    corr_next,
    part_next,
    part_in,
    part,
    parts,
    listed,
    listed_next,
    code,
    code_next,
    ghigh,
    glow,
    nhigh,
    nlow,
    scale_row,
    shares,
    shares_prev,
    shares_next,
    shares_second,
    halo_out,
    from_prev,
    from_next,
    gram,
    stage1,
    half,
    stage2,
    in_sems,
    send,
    recv,
    part_send,
    part_recv,
    halo_send,
    halo_recv,
    s1_send,
    s1_recv,
    s2_send,
    s2_recv,
):
    groups, plane, planes, scale_factor = sizes
    count = plane * planes
    subjects, voxels, frames = series_ref.shape
    offsets = near_ref.shape[0]
    vecs = start_ref.shape[0]
    halves, width = 2 * subjects, frames // 2
    passed = zahead.shape[0]
    me = lax.axis_index("vox")
    group = lax.axis_index("subj")
    core = lax.rem(me, 2)
    spot = lax.rem(me, plane)
    level = me // plane
    following = {"vox": lax.rem(me + 1, count)}
    previous = {"vox": lax.rem(me + count - 1, count)}
    second = {"vox": lax.rem(me + count - 2, count)}

    plane_peers = [lax.rem(spot + d, plane) for d in range(1, plane)]
    level_peers = [lax.rem(level + d, planes) for d in range(1, planes)]
    group_peers = [lax.rem(group + d, groups) for d in range(1, groups)]

    barrier = pltpu.get_barrier_semaphore()
    def far_first(peers):
        return sorted(range(len(peers)), key=lambda d: -min(d + 1, len(peers) - d))

    targets = []
    for d in far_first(range(max(groups, planes) - 1)):
        if d < groups - 1:
            targets.append({"subj": group_peers[d]})
        if d < planes - 1:
            targets.append({"vox": level_peers[d] * plane + spot})
    targets += [following, previous, {"vox": lax.rem(me + 2, count)}, second]
    targets += [{"vox": level * plane + p} for p in plane_peers]
    for target in targets:
        pl.semaphore_signal(
            barrier, inc=1, device_id=target, device_id_type=pl.DeviceIdType.MESH
        )

    loads = [
        pltpu.make_async_copy(series_ref.at[s], raw.at[s], in_sems.at[s])
        for s in range(subjects)
    ]
    small = [
        pltpu.make_async_copy(near_ref, near, in_sems.at[subjects]),
        pltpu.make_async_copy(mask_ref, live, in_sems.at[subjects + 1]),
        pltpu.make_async_copy(start_ref, begin, in_sems.at[subjects + 2]),
    ]
    for load in loads + small:
        load.start()

    def remote(src, dst, send_sem, recv_sem, target):
        return pltpu.make_async_remote_copy(
            src_ref=src,
            dst_ref=dst,
            send_sem=send_sem,
            recv_sem=recv_sem,
            device_id=target,
            device_id_type=pl.DeviceIdType.MESH,
        )

    def single(index, src, dst, target):
        return remote(src, dst, send.at[index], recv.at[index], target)

    def standardize(s):
        step = 64
        for r in range(0, voxels, step):
            values = raw[s, r : r + step, :].astype(jnp.float32)
            center = values - jnp.mean(values, axis=-1, keepdims=True)
            spread = jnp.mean(center * center, axis=-1, keepdims=True)
            result = (center * lax.rsqrt(spread + 1e-05)).astype(jnp.bfloat16)
            zown[2 * s, r : r + step, :] = result[:, :width]
            zown[2 * s + 1, r : r + step, :] = result[:, width:]

    with jax.named_scope("zscore"):
        for s in range(subjects):
            loads[s].wait()
            standardize(s)
        for load in small:
            load.wait()
    with jax.named_scope("barrier"):
        pl.semaphore_wait(barrier, len(targets))
    split_at = halves - passed - 1
    back_copy = single(2, zown.at[passed : halves - 1], zback.at[0:split_at], previous)
    back_last = single(
        10, zown.at[halves - 1 : halves], zback.at[split_at : split_at + 1], previous
    )
    first_on = single(0, zown.at[0:2], zahead.at[0:2], following)
    rest_on = single(1, zown.at[2 : passed - 1], zahead.at[2 : passed - 1], following)
    last_on = single(9, zown.at[passed - 1 : passed], zahead.at[passed - 1 : passed], following)
    near_copy = single(3, near, near_next, previous)
    ons = [first_on, rest_on, last_on]
    backs = [near_copy, back_copy, back_last]

    def start_for(parity, copies):
        @pl.when(core == parity)
        def _():
            for copy in copies:
                copy.start()

    start_for(1, ons)
    start_for(0, backs)

    def products(left, right, first, last, left_first=0, right_first=0):
        total = None
        for h in range(first, last):
            term = matmul(left[left_first + h], right[right_first + h], NT)
            total = term if total is None else total + term
        return total

    tile = lax.broadcasted_iota(jnp.int32, (8, voxels), 0)

    def slots_of(ref):
        return [jnp.broadcast_to(ref[k : k + 1, :], (8, voxels)) for k in range(offsets)]

    def gathered(source, index):
        return jnp.concatenate(
            [
                jnp.take_along_axis(
                    source[:, c : c + 128], index[:, c : c + 128], axis=0,
                    mode="promise_in_bounds",
                )
                for c in range(0, voxels, 128)
            ],
            axis=1,
        )

    def picked(source, table, first, last, sums):
        rest = jnp.full((16 - offsets, voxels), -1, jnp.int32)
        slots = [table[:8, :], jnp.concatenate([table[8:offsets, :], rest], axis=0)]
        inner = [slot & 7 for slot in slots]
        outer = [lax.shift_right_arithmetic(slot, 3) for slot in slots]

        def body(r, sums):
            values = source[pl.ds(pl.multiple_of(r * 8, 8), 8), :]
            return tuple(
                jnp.where(outer[h] == r, gathered(values, inner[h]), total)
                for h, total in enumerate(sums)
            )

        return lax.fori_loop(first // 8, last // 8, body, sums, unroll=4)

    def down(sums, target):
        target[:8, :] = sums[0]
        target[8:offsets, :] = sums[1][: offsets - 8]

    def number_edges(slots, codes, rows_total):
        @pl.loop(0, rows_total // 8)
        def _(r):
            ids = tile + r * 8
            number = jnp.full((8, voxels), 15, jnp.int32)
            for k in range(offsets):
                number = jnp.where(ids == slots[k], k, number)
            codes[pl.ds(pl.multiple_of(r * 8, 8), 8), :] = number

    nothing = tuple(jnp.zeros((8, voxels), jnp.float32) for _ in range(2))
    with jax.named_scope("pick_own"):
        corr[voxels:, :] = products(zown, zown, 0, halves)
        sums = picked(corr, near, voxels, 2 * voxels, nothing)
        vectors = live[...].astype(jnp.float32) * begin[...]
        halo_out[0] = vectors
    start_for(0, ons)
    start_for(1, backs)
    number_edges(slots_of(near), code, 2 * voxels)
    with jax.named_scope("wait_first"):
        first_on.wait_recv()
    corr[:voxels, :] = products(zahead, zown, 0, 2)
    with jax.named_scope("wait_back"):
        near_copy.wait_recv()
        back_copy.wait_recv()
    corr_next[...] = products(zown, zback, 0, split_at, left_first=passed)
    with jax.named_scope("wait_back_last"):
        back_last.wait_recv()
    with jax.named_scope("pick_next"):
        corr_next[...] += products(zown, zback, split_at, split_at + 1, left_first=passed)
        down(picked(corr_next, near_next, 0, voxels, nothing), part_next)
    next_copy = single(4, part_next, part_in, following)
    next_copy.start()
    number_edges(slots_of(near_next), code_next, voxels)
    with jax.named_scope("wait_rest"):
        rest_on.wait_recv()
    corr[:voxels, :] += products(zahead, zown, 2, passed - 1)
    with jax.named_scope("wait_last"):
        last_on.wait_recv()
    with jax.named_scope("pick_cross"):
        corr[:voxels, :] += products(zahead, zown, passed - 1, passed)
        down(picked(corr, near, 0, voxels, sums), part)
    with jax.named_scope("wait_part"):
        next_copy.wait_recv()
    part[...] += part_in[...]

    part_copies = []
    for d in far_first(group_peers):
        copy = remote(
            part, parts.at[group], part_send.at[d], part_recv.at[group], {"subj": group_peers[d]}
        )
        copy.start()
        part_copies.append(copy)

    def halo(t):
        return (
            remote(halo_out.at[t], from_prev.at[t], halo_send.at[t, 0], halo_recv.at[t, 0], following),
            remote(halo_out.at[t], from_next.at[t], halo_send.at[t, 1], halo_recv.at[t, 1], previous),
        )

    for copy in halo(0):
        copy.start()
    parts[group] = part[...]
    with jax.named_scope("subj_wait"):
        for d, peer in enumerate(group_peers):
            remote(
                part, parts.at[peer], part_send.at[d], part_recv.at[peer], {"subj": peer}
            ).wait_recv()
    summed = parts[0]
    for g in range(1, groups):
        summed = summed + parts[g]
    weight = jnp.where(near[...] >= 0, jnp.exp(scale_factor * summed), 0.0)
    listed[...] = weight
    list_copy = single(5, listed, listed_next, previous)
    list_copy.start()

    def dense(codes, weight_table, high_out, low_out, rows_total):
        first = weight_table[:8, :]
        second_rows = jnp.concatenate(
            [weight_table[8:offsets, :], jnp.zeros((16 - offsets, voxels), jnp.float32)], axis=0
        )

        @pl.loop(0, rows_total // 16, unroll=2)
        def _(r):
            tiles = []
            for h in range(2):
                number = codes[pl.ds(pl.multiple_of(r * 16 + h * 8, 8), 8), :]
                inner = number & 7
                tiles.append(
                    jnp.where(number < 8, gathered(first, inner), gathered(second_rows, inner))
                )
            high, low = split(jnp.concatenate(tiles, axis=0))
            rows = pl.ds(pl.multiple_of(r * 16, 16), 16)
            high_out[rows, :] = high
            low_out[rows, :] = low

    ones = jnp.ones((8, voxels), jnp.bfloat16)
    with jax.named_scope("dense"):
        dense(code, listed, ghigh, glow, 2 * voxels)
        owed = matmul(ones, ghigh[...], NT) + matmul(ones, glow[...], NT)
        shares[:1, :] = (
            1.0 + jnp.sum(listed[...], axis=0, keepdims=True) + owed[:1, voxels:]
        )
        shares[1:2, :] = owed[:1, :voxels]
    share_copies = [
        single(6, shares, shares_prev, following),
        single(7, shares, shares_next, previous),
        single(8, shares, shares_second, second),
    ]
    for copy in share_copies:
        copy.start()
    with jax.named_scope("wait_list"):
        list_copy.wait_recv()
    with jax.named_scope("dense_next"):
        dense(code_next, listed_next, nhigh, nlow, voxels)

    def stacked(values):
        high, low = split(values)
        return high, jnp.concatenate([high, low], axis=0)

    def own_part(current):
        scaled = scale_row[...] * current
        high, both = stacked(scaled)
        mine = matmul(both, ghigh[voxels:, :], NT) + matmul(both, ghigh[voxels:, :], NN)
        rest = matmul(high, glow[voxels:, :], NT) + matmul(high, glow[voxels:, :], NN)
        return scaled + (mine[:vecs] + mine[vecs:] + rest)

    def whole_part(current, own, before, after):
        high, both = stacked(before)
        mine = matmul(both, ghigh[:voxels, :], NN)
        rest = matmul(high, glow[:voxels, :], NN)
        high, both = stacked(after)
        mine = mine + matmul(both, nhigh[...], NT)
        rest = rest + matmul(high, nlow[...], NT)
        total = own + (mine[:vecs] + mine[vecs:] + rest)
        return 0.5 * (current + scale_row[...] * total)

    with jax.named_scope("wait_shares"):
        for copy in share_copies + list(halo(0)):
            copy.wait_recv()
    with jax.named_scope("images0"):
        scale_row[...] = live[...].astype(jnp.float32) * lax.rsqrt(
            shares[:1, :] + shares_next[1:2, :]
        )
        scale_prev = lax.rsqrt(shares_prev[:1, :] + shares[1:2, :])
        scale_next = lax.rsqrt(shares_next[:1, :] + shares_second[1:2, :])
        images = whole_part(
            vectors, own_part(vectors), scale_prev * from_prev[0], scale_next * from_next[0]
        )

    mid = vecs // 2
    lane = lax.broadcasted_iota(jnp.int32, (mid, 2 * vecs), 1)
    row = lax.broadcasted_iota(jnp.int32, (mid, 2 * vecs), 0)
    column = lax.rem(lane, vecs)
    row_all = lax.broadcasted_iota(jnp.int32, (vecs, 2 * vecs), 0)
    lane_all = lax.broadcasted_iota(jnp.int32, (vecs, 2 * vecs), 1)
    identity = (lane_all - vecs == row_all).astype(jnp.float32)
    fold = mid // 2

    def send_halo(t, current):
        halo_out[t] = scale_row[...] * current
        for copy in halo(t):
            copy.start()

    def next_images(t, current, own):
        with jax.named_scope("wait_halo"):
            for copy in halo(t):
                copy.wait_recv()
        return whole_part(current, own, from_prev[t], from_next[t])

    def stage1_copy(t, d, arriving=False):
        peer = plane_peers[d]
        target = {"vox": level * plane + peer}
        slot = peer if arriving else spot
        return remote(gram.at[t], stage1.at[t, slot], s1_send.at[t, d], s1_recv.at[t, slot], target)

    def stage2_copy(t, d, arriving=False):
        peer = level_peers[d]
        target = {"vox": peer * plane + spot}
        slot = peer if arriving else level
        return remote(half.at[t], stage2.at[t, slot], s2_send.at[t, d], s2_recv.at[t, slot], target)

    def sum_start(t, current):
        upper, lower = current[:mid], current[mid:]
        first = matmul(upper, jnp.concatenate([upper, lower] * 2, axis=0), NT, HIGHEST)
        last = matmul(lower, jnp.concatenate([lower] * 4, axis=0), NT, HIGHEST)
        square = jnp.where((column < mid) & (row < column), last, first)
        gram[t, : fold, :] = jnp.where(lane[:fold] < vecs, square[:fold], square[fold:])
        gram[t, fold : fold + 1, :] = jnp.sum(
            jnp.where(row == column, last, 0.0), axis=0, keepdims=True
        )
        for d in far_first(plane_peers):
            stage1_copy(t, d).start()
        stage1[t, spot] = gram[t]

    def sum_planes(t):
        with jax.named_scope(f"s1_wait{t}"):
            for d in range(plane - 1):
                stage1_copy(t, d, True).wait_recv()
        total = stage1[t, 0]
        for p in range(1, plane):
            total = total + stage1[t, p]
        half[t] = total
        for d in far_first(level_peers):
            stage2_copy(t, d).start()
        stage2[t, level] = total

    def sum_end(t):
        with jax.named_scope(f"s2_wait{t}"):
            for d in range(planes - 1):
                stage2_copy(t, d, True).wait_recv()
        total = stage2[t, 0]
        for p in range(1, planes):
            total = total + stage2[t, p]
        folded, diagonal = total[:fold], total[fold : fold + 1]
        square = jnp.concatenate([folded, pltpu.roll(folded, vecs, 1)], axis=0)
        filled = jnp.concatenate(
            [square, jnp.zeros((2 * vecs - mid, 2 * vecs), jnp.float32)], axis=0
        )
        turned = filled.T
        top = jnp.where((lane < mid) & (row < lane), turned[:mid], square)
        corner = jnp.where(row < lane, square, jnp.where(row == lane, diagonal, turned[:mid]))
        bottom = jnp.where(lane < mid, turned[mid:vecs], pltpu.roll(corner, mid, 1))
        return jnp.concatenate([top, bottom], axis=0)

    def inverse_factor(matrix):
        solved = factor_inverse(jnp.where(lane_all < vecs, matrix, identity))
        return pltpu.roll(solved, vecs, 1)[:, :vecs]

    def normalized(inverse, matrix):
        left = matmul(inverse, matrix[:, :vecs], NN, HIGHEST)
        padded = jnp.concatenate([inverse, jnp.zeros_like(inverse)], axis=0)
        return matmul(left, padded, NT, HIGHEST)

    sum_start(0, images)
    send_halo(1, images)
    own = own_part(images)
    sum_planes(0)
    ahead = next_images(1, images, own)
    sum_start(1, ahead)
    send_halo(2, ahead)
    own = own_part(ahead)
    matrix = sum_end(0)
    sum_planes(1)
    with jax.named_scope("chol0"):
        inverse = inverse_factor(matrix)
    with jax.named_scope("images2"):
        images = matmul(inverse, next_images(2, ahead, own), NN, HIGHEST)
        sum_start(2, images)
    sum_planes(2)
    matrix = sum_end(1)
    with jax.named_scope("chol1"):
        inverse = inverse_factor(normalized(inverse, matrix))
    images = matmul(inverse, images, NN, HIGHEST)
    singles = [first_on, rest_on, last_on, back_copy, back_last, near_copy, next_copy]
    for copy in singles + [list_copy] + share_copies + part_copies:
        copy.wait_send()
    for t in range(ITERS):
        for copy in halo(t):
            copy.wait_send()
        for d in range(plane - 1):
            stage1_copy(t, d).wait_send()
        for d in range(planes - 1 if t < ITERS - 1 else 0):
            stage2_copy(t, d).wait_send()
    matrix = sum_end(2)
    with jax.named_scope("chol2"):
        inverse = inverse_factor(normalized(inverse, matrix))
    out_ref[...] = matmul(inverse, images, NN, HIGHEST)
    for d in range(planes - 1):
        stage2_copy(ITERS - 1, d).wait_send()


def solution(mesh):
    count, groups = mesh.shape["vox"], mesh.shape["subj"]
    plane = 8 if count >= 16 else count // 2
    planes = count // plane

    def on_device(series, live_mask, neighbours, start_vectors):
        subjects, voxels, frames = series.shape
        vecs = start_vectors.shape[1]
        offsets = neighbours.shape[1]
        scale_factor = 0.5 / math.sqrt(frames * subjects * groups)
        f32, bf16, i32 = jnp.float32, jnp.bfloat16, jnp.int32
        block = (vecs, voxels)
        table = (offsets, voxels)
        line = (1, voxels)
        packed = (vecs // 4 + 1, 2 * vecs)
        halves, width = 2 * subjects, frames // 2
        passed = halves * 5 // 8
        dma = pltpu.SemaphoreType.DMA
        outside = pl.BlockSpec(memory_space=pltpu.HBM)
        result = pl.pallas_call(
            functools.partial(kernel, (groups, plane, planes, scale_factor)),
            out_shape=jax.ShapeDtypeStruct(block, f32),
            in_specs=[outside] * 4,
            out_specs=pl.BlockSpec(memory_space=pltpu.VMEM),
            scratch_shapes=[
                pltpu.VMEM((subjects, voxels, frames), bf16),
                pltpu.VMEM((halves, voxels, width), bf16),
                pltpu.VMEM((passed, voxels, width), bf16),
                pltpu.VMEM((halves - passed, voxels, width), bf16),
                pltpu.VMEM(table, i32),
                pltpu.VMEM(table, i32),
                pltpu.VMEM(line, i32),
                pltpu.VMEM(block, f32),
                pltpu.VMEM((2 * voxels, voxels), f32),
                pltpu.VMEM((voxels, voxels), f32),
                pltpu.VMEM(table, f32),
                pltpu.VMEM(table, f32),
                pltpu.VMEM(table, f32),
                pltpu.VMEM((groups, *table), f32),
                pltpu.VMEM(table, f32),
                pltpu.VMEM(table, f32),
                pltpu.VMEM((2 * voxels, voxels), i32),
                pltpu.VMEM((voxels, voxels), i32),
                pltpu.VMEM((2 * voxels, voxels), bf16),
                pltpu.VMEM((2 * voxels, voxels), bf16),
                pltpu.VMEM((voxels, voxels), bf16),
                pltpu.VMEM((voxels, voxels), bf16),
                pltpu.VMEM(line, f32),
                pltpu.VMEM((2, voxels), f32),
                pltpu.VMEM((2, voxels), f32),
                pltpu.VMEM((2, voxels), f32),
                pltpu.VMEM((2, voxels), f32),
                pltpu.VMEM((ITERS, *block), f32),
                pltpu.VMEM((ITERS, *block), f32),
                pltpu.VMEM((ITERS, *block), f32),
                pltpu.VMEM((ITERS, *packed), f32),
                pltpu.VMEM((ITERS, plane, *packed), f32),
                pltpu.VMEM((ITERS, *packed), f32),
                pltpu.VMEM((ITERS, planes, *packed), f32),
                dma((subjects + 3,)),
                dma((11,)),
                dma((11,)),
                dma((max(groups - 1, 1),)),
                dma((groups,)),
                dma((ITERS, 2)),
                dma((ITERS, 2)),
                dma((ITERS, plane - 1)),
                dma((ITERS, plane)),
                dma((ITERS, planes - 1)),
                dma((ITERS, planes)),
            ],
            compiler_params=pltpu.CompilerParams(
                collective_id=0, has_side_effects=True, vmem_limit_bytes=32 << 20
            ),
        )(
            *(
                pltpu.with_memory_space_constraint(operand, pltpu.HBM)
                for operand in (
                    series, live_mask.reshape(1, voxels), neighbours.T, start_vectors.T
                )
            )
        )
        return result.T

    placed = (P("subj", "vox", None), P("vox"), P("vox", None), P("vox", None))
    return jax.shard_map(
        on_device, mesh=mesh, in_specs=placed, out_specs=P("vox", None), check_vma=False
    )
```

```python
import functools
import math

import jax
import jax.numpy as jnp
from jax import lax
from jax.experimental import pallas as pl
from jax.experimental.pallas import tpu as pltpu
from jax.sharding import PartitionSpec as P

ITERS = 3
HIGHEST = lax.Precision.HIGHEST
NN = (((1,), (0,)), ((), ()))
NT = (((1,), (1,)), ((), ()))


def matmul(left, right, dims, precision=None):
    return lax.dot_general(
        left, right, dims, precision=precision, preferred_element_type=jnp.float32
    )


def split(values):
    high = values.astype(jnp.bfloat16)
    low = (values - high.astype(jnp.float32)).astype(jnp.bfloat16)
    return high, low


def factor_inverse(rows):
    total, width = rows.shape
    sublane = lax.broadcasted_iota(jnp.int32, (8, width), 0)

    def spread(first, left):
        return [
            jnp.broadcast_to(rows[:, first + c : first + c + 1], (left, width))
            for c in range(8)
        ]

    done = []
    cols = spread(0, total)
    for first in range(0, total, 8):
        left = total - first
        more = first + 8 < total
        if more:
            cols = cols + spread(first + 8, left)
        block = jnp.zeros((8, width), jnp.float32)
        for c in range(8):
            root = lax.rsqrt(cols[c][c : c + 1, :])
            lower = cols[c] * root
            pivot = rows[c : c + 1, :] * root
            block = jnp.where(sublane == c, pivot, block)
            rows = rows - lower * pivot
            for other in range(c + 1, len(cols)):
                cols[other] = cols[other] - lower * lower[other : other + 1, :]
        done.append(block)
        rows = rows[8:]
        cols = [column[8:] for column in cols[8:]]
    return jnp.concatenate(done, axis=0)


def kernel(
    sizes,
    series_ref,
    mask_ref,
    near_ref,
    start_ref,
    out_ref,
    raw,
    zown,
    zahead,
    zback,
    near,
    near_next,
    live,
    begin,
    corr,
    corr_next,
    part_next,
    part_in,
    part,
    parts,
    listed,
    listed_next,
    code,
    code_next,
    ghigh,
    glow,
    nhigh,
    nlow,
    scale_row,
    shares,
    shares_prev,
    shares_next,
    shares_second,
    halo_out,
    from_prev,
    from_next,
    gram,
    stage1,
    half,
    stage2,
    in_sems,
    send,
    recv,
    part_send,
    part_recv,
    halo_send,
    halo_recv,
    s1_send,
    s1_recv,
    s2_send,
    s2_recv,
):
    groups, plane, planes, scale_factor = sizes
    count = plane * planes
    subjects, voxels, frames = series_ref.shape
    offsets = near_ref.shape[0]
    vecs = start_ref.shape[0]
    halves, width = 2 * subjects, frames // 2
    passed = zahead.shape[0]
    me = lax.axis_index("vox")
    group = lax.axis_index("subj")
    core = lax.rem(me, 2)
    spot = lax.rem(me, plane)
    level = me // plane
    following = {"vox": lax.rem(me + 1, count)}
    previous = {"vox": lax.rem(me + count - 1, count)}
    second = {"vox": lax.rem(me + count - 2, count)}

    plane_peers = [lax.rem(spot + d, plane) for d in range(1, plane)]
    level_peers = [lax.rem(level + d, planes) for d in range(1, planes)]
    group_peers = [lax.rem(group + d, groups) for d in range(1, groups)]

    barrier = pltpu.get_barrier_semaphore()
    def far_first(peers):
        return sorted(range(len(peers)), key=lambda d: -min(d + 1, len(peers) - d))

    targets = []
    for d in far_first(range(max(groups, planes) - 1)):
        if d < groups - 1:
            targets.append({"subj": group_peers[d]})
        if d < planes - 1:
            targets.append({"vox": level_peers[d] * plane + spot})
    targets += [following, previous, {"vox": lax.rem(me + 2, count)}, second]
    targets += [{"vox": level * plane + p} for p in plane_peers]
    for target in targets:
        pl.semaphore_signal(
            barrier, inc=1, device_id=target, device_id_type=pl.DeviceIdType.MESH
        )

    loads = [
        pltpu.make_async_copy(series_ref.at[s], raw.at[s], in_sems.at[s])
        for s in range(subjects)
    ]
    small = [
        pltpu.make_async_copy(near_ref, near, in_sems.at[subjects]),
        pltpu.make_async_copy(mask_ref, live, in_sems.at[subjects + 1]),
        pltpu.make_async_copy(start_ref, begin, in_sems.at[subjects + 2]),
    ]
    for load in loads + small:
        load.start()

    def remote(src, dst, send_sem, recv_sem, target):
        return pltpu.make_async_remote_copy(
            src_ref=src,
            dst_ref=dst,
            send_sem=send_sem,
            recv_sem=recv_sem,
            device_id=target,
            device_id_type=pl.DeviceIdType.MESH,
        )

    def single(index, src, dst, target):
        return remote(src, dst, send.at[index], recv.at[index], target)

    def standardize(s):
        step = 64
        for r in range(0, voxels, step):
            values = raw[s, r : r + step, :].astype(jnp.float32)
            center = values - jnp.mean(values, axis=-1, keepdims=True)
            spread = jnp.mean(center * center, axis=-1, keepdims=True)
            result = (center * lax.rsqrt(spread + 1e-05)).astype(jnp.bfloat16)
            zown[2 * s, r : r + step, :] = result[:, :width]
            zown[2 * s + 1, r : r + step, :] = result[:, width:]

    with jax.named_scope("zscore"):
        for s in range(subjects):
            loads[s].wait()
            standardize(s)
        for load in small:
            load.wait()
    with jax.named_scope("barrier"):
        pl.semaphore_wait(barrier, len(targets))
    split_at = halves - passed - 1
    back_copy = single(2, zown.at[passed : halves - 1], zback.at[0:split_at], previous)
    back_last = single(
        10, zown.at[halves - 1 : halves], zback.at[split_at : split_at + 1], previous
    )
    first_on = single(0, zown.at[0:2], zahead.at[0:2], following)
    rest_on = single(1, zown.at[2 : passed - 1], zahead.at[2 : passed - 1], following)
    last_on = single(9, zown.at[passed - 1 : passed], zahead.at[passed - 1 : passed], following)
    near_copy = single(3, near, near_next, previous)
    ons = [first_on, rest_on, last_on]
    backs = [near_copy, back_copy, back_last]

    def start_for(parity, copies):
        @pl.when(core == parity)
        def _():
            for copy in copies:
                copy.start()

    start_for(1, ons)
    start_for(0, backs)

    def products(left, right, first, last, left_first=0, right_first=0):
        total = None
        for h in range(first, last):
            term = matmul(left[left_first + h], right[right_first + h], NT)
            total = term if total is None else total + term
        return total

    tile = lax.broadcasted_iota(jnp.int32, (8, voxels), 0)

    def slots_of(ref):
        return [jnp.broadcast_to(ref[k : k + 1, :], (8, voxels)) for k in range(offsets)]

    def gathered(source, index):
        return jnp.concatenate(
            [
                jnp.take_along_axis(
                    source[:, c : c + 128], index[:, c : c + 128], axis=0,
                    mode="promise_in_bounds",
                )
                for c in range(0, voxels, 128)
            ],
            axis=1,
        )

    def picked(source, table, first, last, sums):
        rest = jnp.full((16 - offsets, voxels), -1, jnp.int32)
        slots = [table[:8, :], jnp.concatenate([table[8:offsets, :], rest], axis=0)]
        inner = [slot & 7 for slot in slots]
        outer = [lax.shift_right_arithmetic(slot, 3) for slot in slots]

        def body(r, sums):
            values = source[pl.ds(pl.multiple_of(r * 8, 8), 8), :]
            return tuple(
                jnp.where(outer[h] == r, gathered(values, inner[h]), total)
                for h, total in enumerate(sums)
            )

        return lax.fori_loop(first // 8, last // 8, body, sums, unroll=4)

    def down(sums, target):
        target[:8, :] = sums[0]
        target[8:offsets, :] = sums[1][: offsets - 8]

    def number_edges(slots, codes, rows_total):
        @pl.loop(0, rows_total // 8)
        def _(r):
            ids = tile + r * 8
            number = jnp.full((8, voxels), 15, jnp.int32)
            for k in range(offsets):
                number = jnp.where(ids == slots[k], k, number)
            codes[pl.ds(pl.multiple_of(r * 8, 8), 8), :] = number

    nothing = tuple(jnp.zeros((8, voxels), jnp.float32) for _ in range(2))
    with jax.named_scope("pick_own"):
        corr[voxels:, :] = products(zown, zown, 0, halves)
        sums = picked(corr, near, voxels, 2 * voxels, nothing)
        vectors = live[...].astype(jnp.float32) * begin[...]
        halo_out[0] = vectors
    start_for(0, ons)
    start_for(1, backs)
    number_edges(slots_of(near), code, 2 * voxels)
    with jax.named_scope("wait_first"):
        first_on.wait_recv()
    corr[:voxels, :] = products(zahead, zown, 0, 2)
    with jax.named_scope("wait_back"):
        near_copy.wait_recv()
        back_copy.wait_recv()
    corr_next[...] = products(zown, zback, 0, split_at, left_first=passed)
    with jax.named_scope("wait_back_last"):
        back_last.wait_recv()
    with jax.named_scope("pick_next"):
        corr_next[...] += products(zown, zback, split_at, split_at + 1, left_first=passed)
        down(picked(corr_next, near_next, 0, voxels, nothing), part_next)
    next_copy = single(4, part_next, part_in, following)
    next_copy.start()
    number_edges(slots_of(near_next), code_next, voxels)
    with jax.named_scope("wait_rest"):
        rest_on.wait_recv()
    corr[:voxels, :] += products(zahead, zown, 2, passed - 1)
    with jax.named_scope("wait_last"):
        last_on.wait_recv()
    with jax.named_scope("pick_cross"):
        corr[:voxels, :] += products(zahead, zown, passed - 1, passed)
        down(picked(corr, near, 0, voxels, sums), part)
    with jax.named_scope("wait_part"):
        next_copy.wait_recv()
    part[...] += part_in[...]

    part_copies = []
    for d in far_first(group_peers):
        copy = remote(
            part, parts.at[group], part_send.at[d], part_recv.at[group], {"subj": group_peers[d]}
        )
        copy.start()
        part_copies.append(copy)

    def halo(t):
        return (
            remote(halo_out.at[t], from_prev.at[t], halo_send.at[t, 0], halo_recv.at[t, 0], following),
            remote(halo_out.at[t], from_next.at[t], halo_send.at[t, 1], halo_recv.at[t, 1], previous),
        )

    for copy in halo(0):
        copy.start()
    parts[group] = part[...]
    with jax.named_scope("subj_wait"):
        for d, peer in enumerate(group_peers):
            remote(
                part, parts.at[peer], part_send.at[d], part_recv.at[peer], {"subj": peer}
            ).wait_recv()
    summed = parts[0]
    for g in range(1, groups):
        summed = summed + parts[g]
    weight = jnp.where(near[...] >= 0, jnp.exp(scale_factor * summed), 0.0)
    listed[...] = weight
    list_copy = single(5, listed, listed_next, previous)
    list_copy.start()

    def dense(codes, weight_table, high_out, low_out, rows_total):
        first = weight_table[:8, :]
        second_rows = jnp.concatenate(
            [weight_table[8:offsets, :], jnp.zeros((16 - offsets, voxels), jnp.float32)], axis=0
        )

        @pl.loop(0, rows_total // 16, unroll=2)
        def _(r):
            tiles = []
            for h in range(2):
                number = codes[pl.ds(pl.multiple_of(r * 16 + h * 8, 8), 8), :]
                inner = number & 7
                tiles.append(
                    jnp.where(number < 8, gathered(first, inner), gathered(second_rows, inner))
                )
            high, low = split(jnp.concatenate(tiles, axis=0))
            rows = pl.ds(pl.multiple_of(r * 16, 16), 16)
            high_out[rows, :] = high
            low_out[rows, :] = low

    ones = jnp.ones((8, voxels), jnp.bfloat16)
    with jax.named_scope("dense"):
        dense(code, listed, ghigh, glow, 2 * voxels)
        owed = matmul(ones, ghigh[...], NT) + matmul(ones, glow[...], NT)
        shares[:1, :] = (
            1.0 + jnp.sum(listed[...], axis=0, keepdims=True) + owed[:1, voxels:]
        )
        shares[1:2, :] = owed[:1, :voxels]
    share_copies = [
        single(6, shares, shares_prev, following),
        single(7, shares, shares_next, previous),
        single(8, shares, shares_second, second),
    ]
    for copy in share_copies:
        copy.start()
    with jax.named_scope("wait_list"):
        list_copy.wait_recv()
    with jax.named_scope("dense_next"):
        dense(code_next, listed_next, nhigh, nlow, voxels)

    def stacked(values):
        high, low = split(values)
        return high, jnp.concatenate([high, low], axis=0)

    def own_part(current):
        scaled = scale_row[...] * current
        high, both = stacked(scaled)
        mine = matmul(both, ghigh[voxels:, :], NT) + matmul(both, ghigh[voxels:, :], NN)
        rest = matmul(high, glow[voxels:, :], NT) + matmul(high, glow[voxels:, :], NN)
        return scaled + (mine[:vecs] + mine[vecs:] + rest)

    def whole_part(current, own, before, after):
        high, both = stacked(before)
        mine = matmul(both, ghigh[:voxels, :], NN)
        rest = matmul(high, glow[:voxels, :], NN)
        high, both = stacked(after)
        mine = mine + matmul(both, nhigh[...], NT)
        rest = rest + matmul(high, nlow[...], NT)
        total = own + (mine[:vecs] + mine[vecs:] + rest)
        return 0.5 * (current + scale_row[...] * total)

    with jax.named_scope("wait_shares"):
        for copy in share_copies + list(halo(0)):
            copy.wait_recv()
    with jax.named_scope("images0"):
        scale_row[...] = live[...].astype(jnp.float32) * lax.rsqrt(
            shares[:1, :] + shares_next[1:2, :]
        )
        scale_prev = lax.rsqrt(shares_prev[:1, :] + shares[1:2, :])
        scale_next = lax.rsqrt(shares_next[:1, :] + shares_second[1:2, :])
        images = whole_part(
            vectors, own_part(vectors), scale_prev * from_prev[0], scale_next * from_next[0]
        )

    mid = vecs // 2
    lane = lax.broadcasted_iota(jnp.int32, (mid, 2 * vecs), 1)
    row = lax.broadcasted_iota(jnp.int32, (mid, 2 * vecs), 0)
    column = lax.rem(lane, vecs)
    row_all = lax.broadcasted_iota(jnp.int32, (vecs, 2 * vecs), 0)
    lane_all = lax.broadcasted_iota(jnp.int32, (vecs, 2 * vecs), 1)
    identity = (lane_all - vecs == row_all).astype(jnp.float32)
    fold = mid // 2

    def send_halo(t, current):
        halo_out[t] = scale_row[...] * current
        for copy in halo(t):
            copy.start()

    def next_images(t, current, own):
        with jax.named_scope("wait_halo"):
            for copy in halo(t):
                copy.wait_recv()
        return whole_part(current, own, from_prev[t], from_next[t])

    def stage1_copy(t, d, arriving=False):
        peer = plane_peers[d]
        target = {"vox": level * plane + peer}
        slot = peer if arriving else spot
        return remote(gram.at[t], stage1.at[t, slot], s1_send.at[t, d], s1_recv.at[t, slot], target)

    def stage2_copy(t, d, arriving=False):
        peer = level_peers[d]
        target = {"vox": peer * plane + spot}
        slot = peer if arriving else level
        return remote(half.at[t], stage2.at[t, slot], s2_send.at[t, d], s2_recv.at[t, slot], target)

    def sum_start(t, current):
        upper, lower = current[:mid], current[mid:]
        first = matmul(upper, jnp.concatenate([upper, lower] * 2, axis=0), NT, HIGHEST)
        last = matmul(lower, jnp.concatenate([lower] * 4, axis=0), NT, HIGHEST)
        square = jnp.where((column < mid) & (row < column), last, first)
        gram[t, : fold, :] = jnp.where(lane[:fold] < vecs, square[:fold], square[fold:])
        gram[t, fold : fold + 1, :] = jnp.sum(
            jnp.where(row == column, last, 0.0), axis=0, keepdims=True
        )
        for d in far_first(plane_peers):
            stage1_copy(t, d).start()
        stage1[t, spot] = gram[t]

    def sum_planes(t):
        with jax.named_scope(f"s1_wait{t}"):
            for d in range(plane - 1):
                stage1_copy(t, d, True).wait_recv()
        total = stage1[t, 0]
        for p in range(1, plane):
            total = total + stage1[t, p]
        half[t] = total
        for d in far_first(level_peers):
            stage2_copy(t, d).start()
        stage2[t, level] = total

    def sum_end(t):
        with jax.named_scope(f"s2_wait{t}"):
            for d in range(planes - 1):
                stage2_copy(t, d, True).wait_recv()
        total = stage2[t, 0]
        for p in range(1, planes):
            total = total + stage2[t, p]
        folded, diagonal = total[:fold], total[fold : fold + 1]
        square = jnp.concatenate([folded, pltpu.roll(folded, vecs, 1)], axis=0)
        filled = jnp.concatenate(
            [square, jnp.zeros((2 * vecs - mid, 2 * vecs), jnp.float32)], axis=0
        )
        turned = filled.T
        top = jnp.where((lane < mid) & (row < lane), turned[:mid], square)
        corner = jnp.where(row < lane, square, jnp.where(row == lane, diagonal, turned[:mid]))
        bottom = jnp.where(lane < mid, turned[mid:vecs], pltpu.roll(corner, mid, 1))
        return jnp.concatenate([top, bottom], axis=0)

    def inverse_factor(matrix):
        solved = factor_inverse(jnp.where(lane_all < vecs, matrix, identity))
        return pltpu.roll(solved, vecs, 1)[:, :vecs]

    def normalized(inverse, matrix):
        left = matmul(inverse, matrix[:, :vecs], NN, HIGHEST)
        padded = jnp.concatenate([inverse, jnp.zeros_like(inverse)], axis=0)
        return matmul(left, padded, NT, HIGHEST)

    sum_start(0, images)
    send_halo(1, images)
    own = own_part(images)
    sum_planes(0)
    ahead = next_images(1, images, own)
    sum_start(1, ahead)
    send_halo(2, ahead)
    own = own_part(ahead)
    matrix = sum_end(0)
    sum_planes(1)
    beyond = next_images(2, ahead, own)
    inverse = inverse_factor(matrix)
    images = matmul(inverse, beyond, NN, HIGHEST)
    sum_start(2, images)
    sum_planes(2)
    matrix = sum_end(1)
    with jax.named_scope("chol1"):
        inverse = inverse_factor(normalized(inverse, matrix))
    images = matmul(inverse, images, NN, HIGHEST)
    singles = [first_on, rest_on, last_on, back_copy, back_last, near_copy, next_copy]
    for copy in singles + [list_copy] + share_copies + part_copies:
        copy.wait_send()
    for t in range(ITERS):
        for copy in halo(t):
            copy.wait_send()
        for d in range(plane - 1):
            stage1_copy(t, d).wait_send()
        for d in range(planes - 1 if t < ITERS - 1 else 0):
            stage2_copy(t, d).wait_send()
    matrix = sum_end(2)
    with jax.named_scope("chol2"):
        inverse = inverse_factor(normalized(inverse, matrix))
    out_ref[...] = matmul(inverse, images, NN, HIGHEST)
    for d in range(planes - 1):
        stage2_copy(ITERS - 1, d).wait_send()


def solution(mesh):
    count, groups = mesh.shape["vox"], mesh.shape["subj"]
    plane = 8 if count >= 16 else count // 2
    planes = count // plane

    def on_device(series, live_mask, neighbours, start_vectors):
        subjects, voxels, frames = series.shape
        vecs = start_vectors.shape[1]
        offsets = neighbours.shape[1]
        scale_factor = 0.5 / math.sqrt(frames * subjects * groups)
        f32, bf16, i32 = jnp.float32, jnp.bfloat16, jnp.int32
        block = (vecs, voxels)
        table = (offsets, voxels)
        line = (1, voxels)
        packed = (vecs // 4 + 1, 2 * vecs)
        halves, width = 2 * subjects, frames // 2
        passed = halves * 5 // 8
        dma = pltpu.SemaphoreType.DMA
        outside = pl.BlockSpec(memory_space=pltpu.HBM)
        result = pl.pallas_call(
            functools.partial(kernel, (groups, plane, planes, scale_factor)),
            out_shape=jax.ShapeDtypeStruct(block, f32),
            in_specs=[outside] * 4,
            out_specs=pl.BlockSpec(memory_space=pltpu.VMEM),
            scratch_shapes=[
                pltpu.VMEM((subjects, voxels, frames), bf16),
                pltpu.VMEM((halves, voxels, width), bf16),
                pltpu.VMEM((passed, voxels, width), bf16),
                pltpu.VMEM((halves - passed, voxels, width), bf16),
                pltpu.VMEM(table, i32),
                pltpu.VMEM(table, i32),
                pltpu.VMEM(line, i32),
                pltpu.VMEM(block, f32),
                pltpu.VMEM((2 * voxels, voxels), f32),
                pltpu.VMEM((voxels, voxels), f32),
                pltpu.VMEM(table, f32),
                pltpu.VMEM(table, f32),
                pltpu.VMEM(table, f32),
                pltpu.VMEM((groups, *table), f32),
                pltpu.VMEM(table, f32),
                pltpu.VMEM(table, f32),
                pltpu.VMEM((2 * voxels, voxels), i32),
                pltpu.VMEM((voxels, voxels), i32),
                pltpu.VMEM((2 * voxels, voxels), bf16),
                pltpu.VMEM((2 * voxels, voxels), bf16),
                pltpu.VMEM((voxels, voxels), bf16),
                pltpu.VMEM((voxels, voxels), bf16),
                pltpu.VMEM(line, f32),
                pltpu.VMEM((2, voxels), f32),
                pltpu.VMEM((2, voxels), f32),
                pltpu.VMEM((2, voxels), f32),
                pltpu.VMEM((2, voxels), f32),
                pltpu.VMEM((ITERS, *block), f32),
                pltpu.VMEM((ITERS, *block), f32),
                pltpu.VMEM((ITERS, *block), f32),
                pltpu.VMEM((ITERS, *packed), f32),
                pltpu.VMEM((ITERS, plane, *packed), f32),
                pltpu.VMEM((ITERS, *packed), f32),
                pltpu.VMEM((ITERS, planes, *packed), f32),
                dma((subjects + 3,)),
                dma((11,)),
                dma((11,)),
                dma((max(groups - 1, 1),)),
                dma((groups,)),
                dma((ITERS, 2)),
                dma((ITERS, 2)),
                dma((ITERS, plane - 1)),
                dma((ITERS, plane)),
                dma((ITERS, planes - 1)),
                dma((ITERS, planes)),
            ],
            compiler_params=pltpu.CompilerParams(
                collective_id=0, has_side_effects=True, vmem_limit_bytes=32 << 20
            ),
        )(
            *(
                pltpu.with_memory_space_constraint(operand, pltpu.HBM)
                for operand in (
                    series, live_mask.reshape(1, voxels), neighbours.T, start_vectors.T
                )
            )
        )
        return result.T

    placed = (P("subj", "vox", None), P("vox"), P("vox", None), P("vox", None))
    return jax.shard_map(
        on_device, mesh=mesh, in_specs=placed, out_specs=P("vox", None), check_vma=False
    )
```
